8 devices in a mesh: ey: 2 (over z, y), ex: 4 (over x, core).
Axes of the slice: x: 2, y: 2, z: 1, core: 2. Of those that a mesh axis runs over, the one named last changes fastest.
Arguments:
- x: bfloat16 [1024, 2048], P(('ey', 'ex'))
- kv_k: bfloat16 [1024, 512, 1, 128], P(('ey', 'ex'))
- kv_v: bfloat16 [1024, 512, 1, 128], P(('ey', 'ex'))
- lens: int32 [1024], P(('ey', 'ex'))
- topk_idx: int32 [1024, 6], P(('ey', 'ex'))
- gates: float32 [1024, 6], P(('ey', 'ex'))
- ln1: bfloat16 [2048], replicated
- ln2: bfloat16 [2048], replicated
- wq: bfloat16 [2048, 2048], replicated
- wo: bfloat16 [2048, 2048], replicated
- ws1: bfloat16 [2048, 1408], replicated
- ws3: bfloat16 [2048, 1408], replicated
- ws2: bfloat16 [1408, 2048], replicated
- w1: bfloat16 [64, 2048, 1408], P(('ey', 'ex'))
- w3: bfloat16 [64, 2048, 1408], P(('ey', 'ex'))
- w2: bfloat16 [64, 1408, 2048], P(('ey', 'ex'))
Outputs:
- output: bfloat16 [1024, 2048], P(('ey', 'ex'))
All inputs are finite; a program needn't handle non-finite values.
Results may differ from the reference program's by a relative error of at most 0.0124533.
Values are sent between devices in bfloat16 or wider.
A program may use at most 1 GiB of HBM per device.

```python
import jax
import jax.numpy as jnp
from jax import lax

EY = 2
EX = 4
TOKENS = 128
LEN = 512
D = 2048
HEADS = 16
KV_HEADS = 1
HEAD = 128
FF = 1408
EXPERTS = 64
TOP = 6
ROWS_MAX = 2
CAP = 24
EPS = 1e-6
GATE_SCALE = 2.5

NDEV = EY * EX
NT = NDEV * TOKENS
EROW = EXPERTS // EY
NSLOT = EXPERTS * NDEV * CAP


def _normal(key, shape, scale):
    return (scale * jax.random.normal(key, shape, jnp.float32)).astype(jnp.bfloat16)


def _stack(key, n, shape, scale):
    return lax.map(lambda k: _normal(k, shape, scale), jax.random.split(key, n))


def _route(key):
    place_key, token_key = jax.random.split(key)
    places = jax.random.permutation(place_key, jnp.arange(EXPERTS, dtype=jnp.int32))
    half_count = EXPERTS // 2
    upper_span = EXPERTS - 1 - half_count
    offset = places - half_count
    square = offset * offset
    weight = jnp.where(offset < 0, 100 - (square * 78) // (half_count * half_count), 100 + (square * 350) // (upper_span * upper_span)).astype(jnp.uint32)
    row_of = jnp.arange(EXPERTS) // EROW

    def pick_one(one_key):
        order_key, count_key, noise_key = jax.random.split(one_key, 3)
        row_order = jax.random.permutation(order_key, EY)
        rows_used = jax.random.randint(count_key, (), 1, ROWS_MAX + 1)
        allowed = jnp.zeros((EY,), jnp.int32).at[row_order].set((jnp.arange(EY) < rows_used).astype(jnp.int32))
        noise_bits = jax.random.bits(noise_key, (EXPERTS,), jnp.uint32) >> 10
        waiting = jnp.where(allowed[row_of] > 0, noise_bits * weight, jnp.uint32(0xFFFFFFFF))
        return jnp.argsort(waiting)[:TOP]
    return jax.vmap(pick_one)(jax.random.split(token_key, NT)).astype(jnp.int32)


def setup_inputs(seed: int = 0) -> dict:
    ks = jax.random.split(jax.random.key(seed), 16)
    kd = jax.random.split(jax.random.fold_in(jax.random.key(seed), 7), 3)
    hd = HEADS * HEAD
    full = jax.random.uniform(kd[0], (NT,), jnp.float32) < 0.3
    short = jax.random.randint(kd[1], (NT,), 1, LEN // 8 + 1, jnp.int32)
    return {
        'x': _normal(ks[0], (NT, D), 1.0),
        'kv_k': _stack(ks[1], NT, (LEN, KV_HEADS, HEAD), 2.0),
        'kv_v': _stack(ks[2], NT, (LEN, KV_HEADS, HEAD), 1.0),
        'lens': jnp.where(full, LEN, short).astype(jnp.int32),
        'topk_idx': _route(kd[2]),
        'gates': GATE_SCALE * jax.nn.softmax(0.5 * jax.random.normal(ks[5], (NT, TOP), jnp.float32), axis=-1),
        'ln1': (1.0 + 0.1 * jax.random.normal(ks[6], (D,), jnp.float32)).astype(jnp.bfloat16),
        'ln2': (1.0 + 0.1 * jax.random.normal(ks[7], (D,), jnp.float32)).astype(jnp.bfloat16),
        'wq': _normal(ks[8], (D, hd), D ** -0.5),
        'wo': _normal(ks[9], (hd, D), hd ** -0.5),
        'ws1': _normal(ks[10], (D, FF), D ** -0.5),
        'ws3': _normal(ks[11], (D, FF), D ** -0.5),
        'ws2': _normal(ks[12], (FF, D), FF ** -0.5),
        'w1': _stack(ks[13], EXPERTS, (D, FF), D ** -0.5),
        'w3': _stack(ks[14], EXPERTS, (D, FF), D ** -0.5),
        'w2': _stack(ks[15], EXPERTS, (FF, D), FF ** -0.5),
    }


def _rms(v, w):
    v = v.astype(jnp.float32)
    r = lax.rsqrt(jnp.mean(v * v, axis=-1, keepdims=True) + EPS)
    return (v * r * w.astype(jnp.float32)).astype(jnp.bfloat16)


def _ffn(u, w1, w3, w2):
    g = jnp.dot(u, w1, preferred_element_type=jnp.float32)
    v = jnp.dot(u, w3, preferred_element_type=jnp.float32)
    z = (jax.nn.silu(g) * v).astype(jnp.bfloat16)
    return jnp.dot(z, w2, preferred_element_type=jnp.float32).astype(jnp.bfloat16)


def _attn(x, kk, vv, lens, ln1, wq, wo):
    b = x.shape[0]
    a = _rms(x, ln1)
    q = jnp.dot(a, wq, preferred_element_type=jnp.float32).astype(jnp.bfloat16)
    q = q.reshape(b, KV_HEADS, HEADS // KV_HEADS, HEAD).astype(jnp.float32)
    s = jnp.einsum('bkgd,blkd->bkgl', q, kk.astype(jnp.float32)) * HEAD ** -0.5
    valid = jnp.arange(LEN)[None, :] < lens[:, None]
    s = jnp.where(valid[:, None, None, :], s, -jnp.inf)
    p = jax.nn.softmax(s, axis=-1).astype(jnp.bfloat16).astype(jnp.float32)
    o = jnp.einsum('bkgl,blkd->bkgd', p, vv.astype(jnp.float32)).astype(jnp.bfloat16)
    attn = jnp.dot(o.reshape(b, HEADS * HEAD), wo, preferred_element_type=jnp.float32)
    return (x.astype(jnp.float32) + attn).astype(jnp.bfloat16)


def _slots(topk_idx, gates):
    chosen = (topk_idx[:, :, None] == jnp.arange(EXPERTS)[None, None, :]).any(axis=1).astype(jnp.int32)
    chosen = chosen.reshape(NDEV, TOKENS, EXPERTS)
    before = (jnp.cumsum(chosen, axis=1) - chosen).reshape(NT, EXPERTS)
    rank = jnp.take_along_axis(before, topk_idx, axis=1)
    src = (jnp.arange(NT, dtype=jnp.int32) // TOKENS)[:, None]
    pos = jnp.where(rank < CAP, (topk_idx * NDEV + src) * CAP + rank, NSLOT).reshape(-1)
    tok = jnp.broadcast_to(jnp.arange(NT, dtype=jnp.int32)[:, None], (NT, TOP)).reshape(-1)
    slot_tok = jnp.full((NSLOT,), NT, jnp.int32).at[pos].set(tok, mode='drop')
    slot_gate = jnp.zeros((NSLOT,), jnp.float32).at[pos].set(gates.reshape(-1), mode='drop')
    return slot_tok.reshape(EXPERTS, NDEV * CAP), slot_gate.reshape(EXPERTS, NDEV * CAP)


def reference(x, kv_k, kv_v, lens, topk_idx, gates, ln1, ln2, wq, wo, ws1, ws3, ws2, w1, w3, w2):
    per_dev = lambda a: a.reshape((NDEV, TOKENS) + a.shape[1:])
    h = lax.map(lambda t: _attn(t[0], t[1], t[2], t[3], ln1, wq, wo),
                (per_dev(x), per_dev(kv_k), per_dev(kv_v), per_dev(lens))).reshape(NT, D)
    u = _rms(h, ln2)
    slot_tok, slot_gate = _slots(topk_idx, gates)
    u_pad = jnp.concatenate([u, jnp.zeros((1, D), jnp.bfloat16)], axis=0)

    def expert(acc, xs):
        tok, gate, a1, a3, a2 = xs
        e = _ffn(u_pad[tok], a1, a3, a2)
        return acc.at[tok].add(gate[:, None] * e.astype(jnp.float32)), None

    routed, _ = lax.scan(expert, jnp.zeros((NT + 1, D), jnp.float32), (slot_tok, slot_gate, w1, w3, w2))
    y = h.astype(jnp.float32) + _ffn(u, ws1, ws3, ws2).astype(jnp.float32) + routed[:NT]
    return y.astype(jnp.bfloat16)
```

```python
import functools

import jax
import jax.numpy as jnp
from jax import lax
from jax.experimental import pallas as pl
from jax.experimental.pallas import tpu as pltpu
from jax.sharding import PartitionSpec as P

EPS = 1e-6
BF = jnp.bfloat16
F32 = jnp.float32
MESH = pl.DeviceIdType.MESH

NA = 3
NB = 5
NC = 256


def _rms(v, w):
    v = v.astype(F32)
    r = lax.rsqrt(jnp.mean(v * v, axis=-1, keepdims=True) + EPS)
    return (v * r * w.astype(F32)).astype(BF)


def _attn(x, kk, vv, lens, ln1, wq, wo):
    b, l, kvh, dh = kk.shape
    hq = wq.shape[1] // dh
    a = _rms(x, ln1)
    q = jnp.dot(a, wq, preferred_element_type=F32).astype(BF).reshape(b, kvh, hq // kvh, dh)
    s = jnp.einsum('bkgd,blkd->bkgl', q, kk, preferred_element_type=F32) * dh ** -0.5
    valid = jnp.arange(l)[None, :] < lens[:, None]
    s = jnp.where(valid[:, None, None, :], s, -jnp.inf)
    p = jax.nn.softmax(s, axis=-1).astype(BF)
    o = jnp.einsum('bkgl,blkd->bkgd', p, vv, preferred_element_type=F32).astype(BF)
    attn = jnp.dot(o.reshape(b, hq * dh), wo, preferred_element_type=F32)
    return (x.astype(F32) + attn).astype(BF)


def _moe_kernel(dims, u_ref, h_ref, rt_ref, ws1, ws3, ws2, w1, w3, w2, y_ref,
                ug, rt, acc, z, xin, s1h, pg, ring_a, ring_b, fb, acc_s, z_s, base, hv, sib, r_d, r_a, r_b,
                keys, gts, loc_sem, a_sem, b_sem, ag_s, ag_r, fw_s, fw_r, rt_s, rt_r, sb_s, sb_r,
                rd_s, rd_r, ra_s, ra_r, rb_s, rb_r):
    b, d, f, edev, cap, ny, nx, kc, nk, nn = dims
    rows = 8 * cap
    half = 2 * cap
    y = lax.axis_index('ey')
    ex = lax.axis_index('ex')
    x = ex // 2
    c = ex % 2
    me = y * nx + ex
    peers = [(y, 2 * (1 - x) + c), (1 - y, 2 * x + c), (1 - y, 2 * (1 - x) + c), (y, 2 * x + 1 - c)]
    pa = ((1 - c) * y + c * (1 - y), 2 * ((1 - c) * (1 - x) + c * x) + c)
    pb = ((1 - c) * (1 - y) + c * y, 2 * ((1 - c) * x + c * (1 - x)) + c)
    chip = y * 2 + x
    chip_a = pa[0] * 2 + pa[1] // 2
    chip_b = pb[0] * 2 + pb[1] // 2
    chip_d = (1 - y) * 2 + 1 - x
    sibling = peers[3]

    def remote(src, dst, ss, rs, dev):
        return pltpu.make_async_remote_copy(src_ref=src, dst_ref=dst, send_sem=ss, recv_sem=rs,
                                            device_id=dev, device_id_type=MESH)

    def urows(k, dev):
        return ug.at[k, pl.ds(pl.multiple_of(dev * b, b), b)]

    def ag(k, j):
        return remote(u_ref.at[:, pl.ds(k * kc, kc)], urows(k, me), ag_s.at[k, j], ag_r.at[k, j], peers[j])

    def fw(k, j):
        src = peers[j][0] * nx + peers[j][1]
        return remote(urows(k, src), urows(k, src), fw_s.at[k, j], fw_r.at[k, j], sibling)

    def rts(i):
        t = lax.rem(me + i, 8)
        return remote(rt_ref, rt.at[me], rt_s.at[i - 1], rt_r.at[i - 1], (t // nx, lax.rem(t, nx)))

    def copy_a(t, k, e):
        slot = t % NA if isinstance(t, int) else lax.rem(t, NA)
        ks = pl.ds(k * kc if isinstance(k, int) else pl.multiple_of(k * kc, kc), kc)
        s1 = ws1.at[ks] if e is None else w1.at[e, ks]
        s3 = ws3.at[ks] if e is None else w3.at[e, ks]
        return (pltpu.make_async_copy(s1, ring_a.at[slot, :, pl.ds(0, f)], a_sem.at[slot, 0]),
                pltpu.make_async_copy(s3, ring_a.at[slot, :, pl.ds(f, f)], a_sem.at[slot, 1]))

    def copy_b(t, n, e):
        slot = t % NB if isinstance(t, int) else lax.rem(t, NB)
        ns = pl.ds(n * NC if isinstance(n, int) else pl.multiple_of(n * NC, NC), NC)
        src = ws2.at[:, ns] if e is None else w2.at[e, :, ns]
        return pltpu.make_async_copy(src, ring_b.at[slot], b_sem.at[slot])

    def start_a(t):
        for q in (copy_a(t, t, None) if t < nk else copy_a(t, (t - nk) // edev, (t - nk) % edev)):
            q.start()

    def start_b(t):
        (copy_b(t, t, None) if t < nn else copy_b(t, (t - nn) // edev, (t - nn) % edev)).start()

    for t in range(NA):
        start_a(t)
    for t in range(NB):
        start_b(t)
    own = [pltpu.make_async_copy(u_ref.at[:, pl.ds(k * kc, kc)], urows(k, me), loc_sem.at[k]) for k in range(nk)]
    for q in own:
        q.start()
    own_h = pltpu.make_async_copy(h_ref, hv, loc_sem.at[nk])
    own_h.start()
    own_rt = pltpu.make_async_copy(rt_ref, rt.at[me], loc_sem.at[nk + 1])
    own_rt.start()

    barrier = pltpu.get_barrier_semaphore()
    for i in range(1, 8):
        t = lax.rem(me + i, 8)
        pl.semaphore_signal(barrier, inc=1, device_id=(t // nx, lax.rem(t, nx)), device_id_type=MESH)
    pl.semaphore_wait(barrier, 7)

    for i in range(1, 8):
        rts(i).start()
    for k in range(nk):
        for j in range(4):
            ag(k, j).start()

    for q in own:
        q.wait()
    for t in range(nk):
        for q in copy_a(t, t, None):
            q.wait()
        r = jnp.dot(ug[t, pl.ds(pl.multiple_of(me * b, b), b), :], ring_a[t % NA], preferred_element_type=F32)
        if t == 0:
            acc_s[...] = r
        else:
            acc_s[...] += r
        start_a(t + NA)

    def swiglu(g, v):
        return (g * (1.0 / (1.0 + jnp.exp(-g))) * v).astype(BF)

    z_s[...] = swiglu(acc_s[:, :f], acc_s[:, f:])

    own_rt.wait()
    for i in range(1, 8):
        rts(i).wait_recv()
    for s in range(8):
        tk = rt[s, 0:8, :]
        gt = rt[s, 8:16, :]
        for e in range(edev):
            m = tk == (me * edev + e).astype(F32)
            keys[s * edev + e:s * edev + e + 1, :] = jnp.sum(jnp.where(m, 1.0, 0.0), axis=0, keepdims=True)
            gts[s * edev + e:s * edev + e + 1, :] = jnp.sum(jnp.where(m, gt, 0.0), axis=0, keepdims=True)
    chosen = keys[...]
    before = (lax.broadcasted_iota(jnp.int32, (b, b), 0) < lax.broadcasted_iota(jnp.int32, (b, b), 1))
    rank = jnp.dot(chosen.astype(BF), jnp.where(before, 1.0, 0.0).astype(BF), preferred_element_type=F32)
    keys[...] = jnp.where(chosen > 0.0, rank, -1.0)
    slot_no = lax.broadcasted_iota(jnp.int32, (cap, b), 0).astype(F32)
    zero = jnp.zeros((cap, b), F32)
    for p in range(4):
        parts = []
        for e in range(edev):
            i0, i1 = 2 * p * edev + e, (2 * p + 1) * edev + e
            one0 = jnp.where(keys[i0:i0 + 1, :] == slot_no, 1.0, 0.0)
            one1 = jnp.where(keys[i1:i1 + 1, :] == slot_no, 1.0, 0.0)
            s1h[p, e * half:(e + 1) * half, :] = jnp.concatenate(
                [jnp.concatenate([one0, zero], axis=1), jnp.concatenate([zero, one1], axis=1)], axis=0).astype(BF)
            parts.append(jnp.concatenate(
                [jnp.concatenate([one0 * gts[i0:i0 + 1, :], zero], axis=1),
                 jnp.concatenate([zero, one1 * gts[i1:i1 + 1, :]], axis=1)], axis=0))
        g = jnp.concatenate(parts, axis=0).T
        hi = g.astype(BF)
        rest = g - hi.astype(F32)
        mid = rest.astype(BF)
        lo = (rest - mid.astype(F32)).astype(BF)
        pg[p, 0:2 * b, :] = hi
        pg[p, 2 * b:4 * b, :] = mid
        pg[p, 4 * b:6 * b, :] = lo

    own_h.wait()
    for n in range(nn):
        copy_b(n, n, None).wait()
        sh = jnp.dot(z_s[...], ring_b[n % NB], preferred_element_type=F32).astype(BF).astype(F32)
        base[n] = hv[:, n * NC:(n + 1) * NC].astype(F32) + sh
        start_b(n + NB)

    def forward(k):
        for j in range(3):
            ag(k, j).wait_recv()
            fw(k, j).start()

    forward(0)
    for k in range(nk):
        ag(k, 3).wait_recv()
        for j in range(3):
            fw(k, j).wait_recv()
        for p in range(4):
            dsp = jnp.dot(s1h[p], ug[k, p * 2 * b:(p + 1) * 2 * b, :], preferred_element_type=F32).astype(BF)
            for e in range(edev):
                xin[e, p * half:(p + 1) * half, :] = dsp[e * half:(e + 1) * half]

        def expert(e, carry, k=k):
            i = k * edev + e
            t = i + nk
            slot = lax.rem(t, NA)
            for q in copy_a(t, k, e):
                q.wait()
            rs = pl.ds(pl.multiple_of(e * rows, rows), rows)
            r = jnp.dot(xin[e], ring_a[slot], preferred_element_type=F32)
            if k == 0:
                acc[rs, :] = r
            else:
                acc[rs, :] += r

            @pl.when(i + NA < nk * edev)
            def _():
                i2 = i + NA
                for q in copy_a(t + NA, i2 // edev, lax.rem(i2, edev)):
                    q.start()
            if k == nk - 1:
                z[e] = swiglu(acc[rs, pl.ds(0, f)], acc[rs, pl.ds(f, f)])
            return carry
        if k + 1 < nk:
            lax.fori_loop(0, edev - 2, expert, 0)
            forward(k + 1)
            lax.fori_loop(edev - 2, edev, expert, 0)
        else:
            lax.fori_loop(0, edev, expert, 0)

    def part(n, core, p):
        col = (core * 4 + p) * NC
        col = col if isinstance(col, int) else pl.multiple_of(col, NC)
        return (pl.ds(pl.multiple_of(n * b, b), b), pl.ds(col, NC))

    def to_sib(n):
        src = acc.at[pl.ds(pl.multiple_of(n * b, b), b), pl.ds(pl.multiple_of((1 - c) * 4 * NC, 4 * NC), 4 * NC)]
        return remote(src, sib.at[n], sb_s.at[n], sb_r.at[n], sibling)

    def send_d(n):
        return remote(acc.at[part(n, c, chip_d)], r_d.at[n], rd_s.at[n], rd_r.at[n], pa)

    def send_a(n):
        return remote(acc.at[part(n, c, chip_a)], r_a.at[n], ra_s.at[n], ra_r.at[n], pa)

    def send_b(n):
        return remote(acc.at[part(n, c, chip_b)], r_b.at[n], rb_s.at[n], rb_r.at[n], pb)

    def both(n, p):
        return acc[part(n, c, p)] + sib[n, :, pl.ds(pl.multiple_of(p * NC, NC), NC)]

    def stage1(n):
        to_sib(n).wait_recv()
        acc[part(n, c, chip_d)] = both(n, chip_d)
        send_d(n).start()
        acc[part(n, c, chip_a)] = both(n, chip_a)
        send_a(n).start()
        base[n] += both(n, chip)

    def stage2(n):
        send_d(n).wait_recv()
        acc[part(n, c, chip_b)] = both(n, chip_b) + r_d[n]
        send_b(n).start()

    def block(n, carry):
        def down(e, cc):
            i = n * edev + e
            t = i + nn
            slot = lax.rem(t, NB)
            copy_b(t, n, e).wait()
            r = jnp.dot(z[e], ring_b[slot], preferred_element_type=F32).astype(BF)
            for p in range(4):
                fb[p, pl.ds(pl.multiple_of(e * half, half), half), :] = r[p * half:(p + 1) * half]

            @pl.when(i + NB < nn * edev)
            def _():
                i2 = i + NB
                copy_b(t + NB, i2 // edev, lax.rem(i2, edev)).start()
            return cc
        lax.fori_loop(0, edev // 2, down, 0)

        @pl.when(n > 0)
        def _():
            stage1(n - 1)
        lax.fori_loop(edev // 2, edev, down, 0)
        for p in range(4):
            q = jnp.dot(pg[p], fb[p], preferred_element_type=F32)
            q = q[0:2 * b] + q[2 * b:4 * b] + q[4 * b:6 * b]
            for core in range(2):
                acc[part(n, core, p)] = q[core * b:(core + 1) * b]
        to_sib(n).start()

        @pl.when(n > 0)
        def _():
            stage2(n - 1)
        return carry
    lax.fori_loop(0, nn, block, 0)
    stage1(nn - 1)
    stage2(nn - 1)
    for n in range(nn):
        send_a(n).wait_recv()
        send_b(n).wait_recv()
        y_ref[:, n * NC:(n + 1) * NC] = (base[n] + r_a[n] + r_b[n]).astype(BF)
    for i in range(1, 8):
        rts(i).wait_send()
    for k in range(nk):
        for j in range(4):
            ag(k, j).wait_send()
        for j in range(3):
            fw(k, j).wait_send()
    for n in range(nn):
        to_sib(n).wait_send()
        send_d(n).wait_send()
        send_a(n).wait_send()
        send_b(n).wait_send()


def _moe(u, h, rt, ws1, ws3, ws2, w1, w3, w2, ny, nx):
    b, d = u.shape
    edev, _, f = w1.shape
    cap = 24
    kc, nk, nn = 512, d // 512, d // NC
    dims = (b, d, f, edev, cap, ny, nx, kc, nk, nn)
    dma = pltpu.SemaphoreType.DMA
    anys = pl.BlockSpec(memory_space=pl.ANY)
    return pl.pallas_call(
        functools.partial(_moe_kernel, dims),
        out_shape=jax.ShapeDtypeStruct((b, d), BF),
        in_specs=[anys] * 9,
        out_specs=pl.BlockSpec(memory_space=pltpu.VMEM),
        scratch_shapes=[
            pltpu.VMEM((nk, 8 * b, kc), BF),
            pltpu.VMEM((8, 16, b), F32),
            pltpu.VMEM((edev * 8 * cap, 2 * f), F32),
            pltpu.VMEM((edev, 8 * cap, f), BF),
            pltpu.VMEM((edev, 8 * cap, kc), BF),
            pltpu.VMEM((4, edev * 2 * cap, 2 * b), BF),
            pltpu.VMEM((4, 6 * b, edev * 2 * cap), BF),
            pltpu.VMEM((NA, kc, 2 * f), BF),
            pltpu.VMEM((NB, f, NC), BF),
            pltpu.VMEM((4, edev * 2 * cap, NC), BF),
            pltpu.VMEM((b, 2 * f), F32),
            pltpu.VMEM((b, f), BF),
            pltpu.VMEM((nn, b, NC), F32),
            pltpu.VMEM((b, d), BF),
            pltpu.VMEM((nn, b, 4 * NC), F32),
            pltpu.VMEM((nn, b, NC), F32),
            pltpu.VMEM((nn, b, NC), F32),
            pltpu.VMEM((nn, b, NC), F32),
            pltpu.VMEM((8 * edev, b), F32),
            pltpu.VMEM((8 * edev, b), F32),
            dma((nk + 2,)), dma((NA, 2)), dma((NB,)),
            dma((nk, 4)), dma((nk, 4)), dma((nk, 3)), dma((nk, 3)), dma((7,)), dma((7,)),
            dma((nn,)), dma((nn,)), dma((nn,)), dma((nn,)), dma((nn,)), dma((nn,)), dma((nn,)), dma((nn,)),
        ],
        compiler_params=pltpu.CompilerParams(collective_id=0, has_side_effects=True, vmem_limit_bytes=67043328),
        name='moe',
    )(u, h, rt, ws1, ws3, ws2, w1, w3, w2)


def solution(mesh):
    ey, ex = mesh.shape['ey'], mesh.shape['ex']
    rows = P(('ey', 'ex'))
    rep = P()

    def local(x, kv_k, kv_v, lens, topk_idx, gates, ln1, ln2, wq, wo, ws1, ws3, ws2, w1, w3, w2):
        h = _attn(x, kv_k, kv_v, lens, ln1, wq, wo)
        u = _rms(h, ln2)
        pad = ((0, 2), (0, 0))
        rt = jnp.concatenate([jnp.pad(topk_idx.astype(F32).T, pad, constant_values=-1.0), jnp.pad(gates.T, pad)])
        return _moe(u, h, rt, ws1, ws3, ws2, w1, w3, w2, ey, ex)

    return jax.shard_map(
        local, mesh=mesh,
        in_specs=(rows, rows, rows, rows, rows, rows, rep, rep, rep, rep, rep, rep, rep, rows, rows, rows),
        out_specs=rows, check_vma=False)
```

```python
import functools

import jax
import jax.numpy as jnp
from jax import lax
from jax.experimental import pallas as pl
from jax.experimental.pallas import tpu as pltpu
from jax.sharding import PartitionSpec as P

EPS = 1e-6
BF = jnp.bfloat16
F32 = jnp.float32
MESH = pl.DeviceIdType.MESH

NA = 3
NB = 5
NC = 256
UP = 8
UL = 8


def _attn_kernel(dims, lens, x_hbm, ln1, ln2, kk, vv, wq, wo, h_ref, u_ref,
                 kb, vb, wb, q2, o2, xa, xv, shorts, longs, x_sem, k_sem, v_sem, w_sem):
    b, l, dh, hq, d = dims
    sh = 64
    blk = 2 * sh
    cq = d // 4
    top = b * l

    xcopy = pltpu.make_async_copy(x_hbm, xv, x_sem)
    xcopy.start()

    def wcopy(w, i, s):
        return pltpu.make_async_copy(w.at[:, pl.ds(i * cq, cq)], wb.at[:, pl.ds(i * cq, cq)], w_sem.at[s, i])

    for i in range(4):
        wcopy(wq, i, 0).start()

    def srow(i):
        return pl.multiple_of(top - (i // 2 + 1) * blk + lax.rem(i, 2) * sh, sh)

    def kv_s(src, dst, sem, t, i):
        return pltpu.make_async_copy(src.at[t, pl.ds(0, sh)], dst.at[pl.ds(srow(i), sh)], sem.at[0])

    def kv_l(src, dst, sem, t, i):
        return pltpu.make_async_copy(src.at[t], dst.at[pl.ds(pl.multiple_of(i * l, l), l)], sem.at[1])

    def sort_rows(t, c):
        cs, cl = c
        short = lens[t] <= sh
        shorts[cs] = t
        longs[cl] = t

        @pl.when(short)
        def _():
            kv_s(kk, kb, k_sem, t, cs).start()

        @pl.when(jnp.logical_not(short))
        def _():
            kv_l(kk, kb, k_sem, t, cl).start()
        one = short.astype(jnp.int32)
        return cs + one, cl + 1 - one
    ns, nl = lax.fori_loop(0, b, sort_rows, (0, 0))
    odd = lax.rem(ns, 2)

    @pl.when(odd == 1)
    def _():
        kv_s(kk, kb, k_sem, shorts[ns - 1], ns).start()
    last = shorts[jnp.maximum(ns - 1, 0)]
    for j in range(2 * UP):
        shorts[ns + j] = last
    last = longs[jnp.maximum(nl - 1, 0)]
    for j in range(UL):
        longs[nl + j] = last
    ns2 = ns + odd

    def issue_s(i, c):
        kv_s(vv, vb, v_sem, shorts[i], i).start()
        return c
    lax.fori_loop(0, ns2, issue_s, 0)

    def issue_l(i, c):
        kv_l(vv, vb, v_sem, longs[i], i).start()
        return c
    lax.fori_loop(0, nl, issue_l, 0)

    xcopy.wait()
    x = xv[...].astype(F32)
    r = lax.rsqrt(jnp.mean(x * x, axis=-1, keepdims=True) + EPS)
    xa[...] = (x * r * ln1[...].astype(F32)).astype(BF)
    for j in range(4):
        wcopy(wq, j, 0).wait()
        q = jnp.dot(xa[...], wb[:, j * cq:(j + 1) * cq], preferred_element_type=F32)
        for hh in range(cq // dh):
            q2[pl.ds(j * (cq // dh) + hh, b, stride=hq), :] = q[:, hh * dh:(hh + 1) * dh].astype(BF).astype(F32)
        wcopy(wo, j, 1).start()

    def wait_s(i, c):
        kv_s(kk, kb, k_sem, 0, 0).wait()
        kv_s(vv, vb, v_sem, 0, 0).wait()
        return c
    lax.fori_loop(0, ns2, wait_s, 0)

    def wait_l(i, c):
        kv_l(kk, kb, k_sem, 0, 0).wait()
        kv_l(vv, vb, v_sem, 0, 0).wait()
        return c
    lax.fori_loop(0, nl, wait_l, 0)

    def qrows(t):
        return pl.ds(pl.multiple_of(t * hq, hq), hq)

    def normal(s):
        e = jnp.exp(s - jnp.max(s, axis=-1, keepdims=True))
        return (e * (1.0 / jnp.sum(e, axis=-1, keepdims=True))).astype(BF)

    nt = (((1,), (1,)), ((), ()))
    pos2 = lax.broadcasted_iota(jnp.int32, (hq, blk), 1)
    scale = dh ** -0.5

    def pairs(it, c):
        ss, idx = [], []
        for j in range(UP):
            i = jnp.minimum(it * UP + j, (ns2 // 2) - 1)
            t0, t1 = shorts[2 * i], shorts[2 * i + 1]
            q = jnp.concatenate([q2[qrows(t0), :], q2[qrows(t1), :]], axis=0).astype(BF)
            kr = pl.ds(pl.multiple_of(top - (i + 1) * blk, blk), blk)
            ss.append(lax.dot_general(q, kb[kr, :], nt, preferred_element_type=F32) * scale)
            idx.append((t0, t1, kr))
        for j in range(UP):
            t0, t1, kr = idx[j]
            s0 = jnp.where(pos2 < lens[t0], ss[j][:hq], -jnp.inf)
            s1 = jnp.where(jnp.logical_and(pos2 >= sh, pos2 < sh + lens[t1]), ss[j][hq:], -jnp.inf)
            o = jnp.dot(normal(jnp.concatenate([s0, s1], axis=0)), vb[kr, :], preferred_element_type=F32)
            o2[qrows(t0), :] = o[:hq]
            o2[qrows(t1), :] = o[hq:]
        return c
    lax.fori_loop(0, (ns2 // 2 + UP - 1) // UP, pairs, 0)

    pos = lax.broadcasted_iota(jnp.int32, (hq, l), 1)

    def single(it, c):
        ss, idx = [], []
        for j in range(UL):
            i = jnp.minimum(it * UL + j, nl - 1)
            t = longs[i]
            kr = pl.ds(pl.multiple_of(i * l, l), l)
            ss.append(lax.dot_general(q2[qrows(t), :].astype(BF), kb[kr, :], nt, preferred_element_type=F32) * scale)
            idx.append((t, kr))
        for j in range(UL):
            t, kr = idx[j]
            p = normal(jnp.where(pos < lens[t], ss[j], -jnp.inf))
            o2[qrows(t), :] = jnp.dot(p, vb[kr, :], preferred_element_type=F32)
        return c
    lax.fori_loop(0, (nl + UL - 1) // UL, single, 0)

    for hh in range(hq):
        xa[:, hh * dh:(hh + 1) * dh] = o2[pl.ds(hh, b, stride=hq), :].astype(BF)
    ssq = jnp.zeros((b, 1), F32)
    for j in range(4):
        cs = slice(j * cq, (j + 1) * cq)
        wcopy(wo, j, 1).wait()
        hv = (xv[:, cs].astype(F32) + jnp.dot(xa[...], wb[:, cs], preferred_element_type=F32)).astype(BF)
        h_ref[:, cs] = hv
        hf = hv.astype(F32)
        ssq += jnp.sum(hf * hf, axis=-1, keepdims=True)
    r = lax.rsqrt(ssq * (1.0 / d) + EPS)
    for j in range(4):
        cs = slice(j * cq, (j + 1) * cq)
        u_ref[:, cs] = (h_ref[:, cs].astype(F32) * r * ln2[:, cs].astype(F32)).astype(BF)


def _attn(x, kk, vv, lens, ln1, ln2, wq, wo):
    b, d = x.shape
    l, dh = kk.shape[1], kk.shape[3]
    hq = wq.shape[1] // dh
    kk, vv = kk.reshape(b, l, dh), vv.reshape(b, l, dh)
    dma = pltpu.SemaphoreType.DMA
    anys = pl.BlockSpec(memory_space=pl.ANY)
    vm = pl.BlockSpec(memory_space=pltpu.VMEM)
    return pl.pallas_call(
        functools.partial(_attn_kernel, (b, l, dh, hq, d)),
        out_shape=(jax.ShapeDtypeStruct((b, d), BF), jax.ShapeDtypeStruct((b, d), BF)),
        in_specs=[pl.BlockSpec(memory_space=pltpu.SMEM), anys, vm, vm, anys, anys, anys, anys],
        out_specs=(vm, vm),
        scratch_shapes=[
            pltpu.VMEM((b * l, dh), BF), pltpu.VMEM((b * l, dh), BF), pltpu.VMEM((d, d), BF),
            pltpu.VMEM((b * hq, dh), F32), pltpu.VMEM((b * hq, dh), F32),
            pltpu.VMEM((b, d), BF), pltpu.VMEM((b, d), BF),
            pltpu.SMEM((b + 2 * UP + 2,), jnp.int32), pltpu.SMEM((b + UL + 2,), jnp.int32),
            dma, dma((2,)), dma((2,)), dma((2, 4)),
        ],
        compiler_params=pltpu.CompilerParams(vmem_limit_bytes=67043328),
        name='attn',
    )(lens, x, ln1.reshape(1, d), ln2.reshape(1, d), kk, vv, wq, wo)


def _moe_kernel(dims, u_ref, h_ref, rt_ref, ws1, ws3, ws2, w1, w3, w2, y_ref,
                ug, rt, acc, z, xin, s1h, pg, ring_a, ring_b, fb, acc_s, z_s, base, hv, sib, r_d, r_a, r_b,
                keys, gts, loc_sem, a_sem, b_sem, ag_s, ag_r, fw_s, fw_r, rt_s, rt_r, sb_s, sb_r,
                rd_s, rd_r, ra_s, ra_r, rb_s, rb_r):
    b, d, f, edev, cap, ny, nx, kc, nk, nn = dims
    rows = 8 * cap
    half = 2 * cap
    y = lax.axis_index('ey')
    ex = lax.axis_index('ex')
    x = ex // 2
    c = ex % 2
    me = y * nx + ex
    peers = [(y, 2 * (1 - x) + c), (1 - y, 2 * x + c), (1 - y, 2 * (1 - x) + c), (y, 2 * x + 1 - c)]
    pa = ((1 - c) * y + c * (1 - y), 2 * ((1 - c) * (1 - x) + c * x) + c)
    pb = ((1 - c) * (1 - y) + c * y, 2 * ((1 - c) * x + c * (1 - x)) + c)
    chip = y * 2 + x
    chip_a = pa[0] * 2 + pa[1] // 2
    chip_b = pb[0] * 2 + pb[1] // 2
    chip_d = (1 - y) * 2 + 1 - x
    sibling = peers[3]

    def remote(src, dst, ss, rs, dev):
        return pltpu.make_async_remote_copy(src_ref=src, dst_ref=dst, send_sem=ss, recv_sem=rs,
                                            device_id=dev, device_id_type=MESH)

    def urows(k, dev):
        return ug.at[k, pl.ds(pl.multiple_of(dev * b, b), b)]

    def ag(k, j):
        return remote(u_ref.at[:, pl.ds(k * kc, kc)], urows(k, me), ag_s.at[k, j], ag_r.at[k, j], peers[j])

    def fw(k, j):
        src = peers[j][0] * nx + peers[j][1]
        return remote(urows(k, src), urows(k, src), fw_s.at[k, j], fw_r.at[k, j], sibling)

    def rts(i):
        t = lax.rem(me + i, 8)
        return remote(rt_ref, rt.at[me], rt_s.at[i - 1], rt_r.at[i - 1], (t // nx, lax.rem(t, nx)))

    def copy_a(t, k, e):
        slot = t % NA if isinstance(t, int) else lax.rem(t, NA)
        ks = pl.ds(k * kc if isinstance(k, int) else pl.multiple_of(k * kc, kc), kc)
        s1 = ws1.at[ks] if e is None else w1.at[e, ks]
        s3 = ws3.at[ks] if e is None else w3.at[e, ks]
        return (pltpu.make_async_copy(s1, ring_a.at[slot, :, pl.ds(0, f)], a_sem.at[slot, 0]),
                pltpu.make_async_copy(s3, ring_a.at[slot, :, pl.ds(f, f)], a_sem.at[slot, 1]))

    def copy_b(t, n, e):
        slot = t % NB if isinstance(t, int) else lax.rem(t, NB)
        ns = pl.ds(n * NC if isinstance(n, int) else pl.multiple_of(n * NC, NC), NC)
        src = ws2.at[:, ns] if e is None else w2.at[e, :, ns]
        return pltpu.make_async_copy(src, ring_b.at[slot], b_sem.at[slot])

    def start_a(t):
        for q in (copy_a(t, t, None) if t < nk else copy_a(t, (t - nk) // edev, (t - nk) % edev)):
            q.start()

    def start_b(t):
        (copy_b(t, t, None) if t < nn else copy_b(t, (t - nn) // edev, (t - nn) % edev)).start()

    for t in range(NA):
        start_a(t)
    for t in range(NB):
        start_b(t)
    own = [pltpu.make_async_copy(u_ref.at[:, pl.ds(k * kc, kc)], urows(k, me), loc_sem.at[k]) for k in range(nk)]
    for q in own:
        q.start()
    own_h = pltpu.make_async_copy(h_ref, hv, loc_sem.at[nk])
    own_h.start()
    own_rt = pltpu.make_async_copy(rt_ref, rt.at[me], loc_sem.at[nk + 1])
    own_rt.start()

    barrier = pltpu.get_barrier_semaphore()
    for i in range(1, 8):
        t = lax.rem(me + i, 8)
        pl.semaphore_signal(barrier, inc=1, device_id=(t // nx, lax.rem(t, nx)), device_id_type=MESH)
    pl.semaphore_wait(barrier, 7)

    for i in range(1, 8):
        rts(i).start()
    for k in range(nk):
        for j in range(4):
            ag(k, j).start()

    for q in own:
        q.wait()
    for t in range(nk):
        for q in copy_a(t, t, None):
            q.wait()
        r = jnp.dot(ug[t, pl.ds(pl.multiple_of(me * b, b), b), :], ring_a[t % NA], preferred_element_type=F32)
        if t == 0:
            acc_s[...] = r
        else:
            acc_s[...] += r
        start_a(t + NA)

    def swiglu(g, v):
        return (g * (1.0 / (1.0 + jnp.exp(-g))) * v).astype(BF)

    z_s[...] = swiglu(acc_s[:, :f], acc_s[:, f:])

    own_rt.wait()
    for i in range(1, 8):
        rts(i).wait_recv()
    for s in range(8):
        tk = rt[s, 0:8, :]
        gt = rt[s, 8:16, :]
        for e in range(edev):
            m = tk == (me * edev + e).astype(F32)
            keys[s * edev + e:s * edev + e + 1, :] = jnp.sum(jnp.where(m, 1.0, 0.0), axis=0, keepdims=True)
            gts[s * edev + e:s * edev + e + 1, :] = jnp.sum(jnp.where(m, gt, 0.0), axis=0, keepdims=True)
    chosen = keys[...]
    before = (lax.broadcasted_iota(jnp.int32, (b, b), 0) < lax.broadcasted_iota(jnp.int32, (b, b), 1))
    rank = jnp.dot(chosen.astype(BF), jnp.where(before, 1.0, 0.0).astype(BF), preferred_element_type=F32)
    keys[...] = jnp.where(chosen > 0.0, rank, -1.0)
    slot_no = lax.broadcasted_iota(jnp.int32, (cap, b), 0).astype(F32)
    zero = jnp.zeros((cap, b), F32)
    for p in range(4):
        parts = []
        for e in range(edev):
            i0, i1 = 2 * p * edev + e, (2 * p + 1) * edev + e
            one0 = jnp.where(keys[i0:i0 + 1, :] == slot_no, 1.0, 0.0)
            one1 = jnp.where(keys[i1:i1 + 1, :] == slot_no, 1.0, 0.0)
            s1h[p, e * half:(e + 1) * half, :] = jnp.concatenate(
                [jnp.concatenate([one0, zero], axis=1), jnp.concatenate([zero, one1], axis=1)], axis=0).astype(BF)
            parts.append(jnp.concatenate(
                [jnp.concatenate([one0 * gts[i0:i0 + 1, :], zero], axis=1),
                 jnp.concatenate([zero, one1 * gts[i1:i1 + 1, :]], axis=1)], axis=0))
        g = jnp.concatenate(parts, axis=0).T
        hi = g.astype(BF)
        rest = g - hi.astype(F32)
        mid = rest.astype(BF)
        lo = (rest - mid.astype(F32)).astype(BF)
        pg[p, 0:2 * b, :] = hi
        pg[p, 2 * b:4 * b, :] = mid
        pg[p, 4 * b:6 * b, :] = lo

    own_h.wait()
    for n in range(nn):
        copy_b(n, n, None).wait()
        sh = jnp.dot(z_s[...], ring_b[n % NB], preferred_element_type=F32).astype(BF).astype(F32)
        base[n] = hv[:, n * NC:(n + 1) * NC].astype(F32) + sh
        start_b(n + NB)

    def forward(k):
        for j in range(3):
            ag(k, j).wait_recv()
            fw(k, j).start()

    forward(0)
    for k in range(nk):
        ag(k, 3).wait_recv()
        for j in range(3):
            fw(k, j).wait_recv()
        for p in range(4):
            dsp = jnp.dot(s1h[p], ug[k, p * 2 * b:(p + 1) * 2 * b, :], preferred_element_type=F32).astype(BF)
            for e in range(edev):
                xin[e, p * half:(p + 1) * half, :] = dsp[e * half:(e + 1) * half]

        def expert(e, carry, k=k):
            i = k * edev + e
            t = i + nk
            slot = lax.rem(t, NA)
            for q in copy_a(t, k, e):
                q.wait()
            rs = pl.ds(pl.multiple_of(e * rows, rows), rows)
            r = jnp.dot(xin[e], ring_a[slot], preferred_element_type=F32)
            if k == 0:
                acc[rs, :] = r
            else:
                acc[rs, :] += r

            @pl.when(i + NA < nk * edev)
            def _():
                i2 = i + NA
                for q in copy_a(t + NA, i2 // edev, lax.rem(i2, edev)):
                    q.start()
            if k == nk - 1:
                z[e] = swiglu(acc[rs, pl.ds(0, f)], acc[rs, pl.ds(f, f)])
            return carry
        if k + 1 < nk:
            lax.fori_loop(0, edev - 2, expert, 0)
            forward(k + 1)
            lax.fori_loop(edev - 2, edev, expert, 0)
        else:
            lax.fori_loop(0, edev, expert, 0)

    def part(n, core, p):
        col = (core * 4 + p) * NC
        col = col if isinstance(col, int) else pl.multiple_of(col, NC)
        return (pl.ds(pl.multiple_of(n * b, b), b), pl.ds(col, NC))

    def to_sib(n):
        src = acc.at[pl.ds(pl.multiple_of(n * b, b), b), pl.ds(pl.multiple_of((1 - c) * 4 * NC, 4 * NC), 4 * NC)]
        return remote(src, sib.at[n], sb_s.at[n], sb_r.at[n], sibling)

    def send_d(n):
        return remote(acc.at[part(n, c, chip_d)], r_d.at[n], rd_s.at[n], rd_r.at[n], pa)

    def send_a(n):
        return remote(acc.at[part(n, c, chip_a)], r_a.at[n], ra_s.at[n], ra_r.at[n], pa)

    def send_b(n):
        return remote(acc.at[part(n, c, chip_b)], r_b.at[n], rb_s.at[n], rb_r.at[n], pb)

    def both(n, p):
        return acc[part(n, c, p)] + sib[n, :, pl.ds(pl.multiple_of(p * NC, NC), NC)]

    def stage1(n):
        to_sib(n).wait_recv()
        acc[part(n, c, chip_d)] = both(n, chip_d)
        send_d(n).start()
        acc[part(n, c, chip_a)] = both(n, chip_a)
        send_a(n).start()
        base[n] += both(n, chip)

    def stage2(n):
        send_d(n).wait_recv()
        acc[part(n, c, chip_b)] = both(n, chip_b) + r_d[n]
        send_b(n).start()

    def block(n, carry):
        def down(e, cc):
            i = n * edev + e
            t = i + nn
            slot = lax.rem(t, NB)
            copy_b(t, n, e).wait()
            r = jnp.dot(z[e], ring_b[slot], preferred_element_type=F32).astype(BF)
            for p in range(4):
                fb[p, pl.ds(pl.multiple_of(e * half, half), half), :] = r[p * half:(p + 1) * half]

            @pl.when(i + NB < nn * edev)
            def _():
                i2 = i + NB
                copy_b(t + NB, i2 // edev, lax.rem(i2, edev)).start()
            return cc
        lax.fori_loop(0, edev // 2, down, 0)

        @pl.when(n > 0)
        def _():
            stage1(n - 1)
        lax.fori_loop(edev // 2, edev, down, 0)
        for p in range(4):
            q = jnp.dot(pg[p], fb[p], preferred_element_type=F32)
            q = q[0:2 * b] + q[2 * b:4 * b] + q[4 * b:6 * b]
            for core in range(2):
                acc[part(n, core, p)] = q[core * b:(core + 1) * b]
        to_sib(n).start()

        @pl.when(n > 0)
        def _():
            stage2(n - 1)
        return carry
    lax.fori_loop(0, nn, block, 0)
    stage1(nn - 1)
    stage2(nn - 1)
    for n in range(nn):
        send_a(n).wait_recv()
        send_b(n).wait_recv()
        y_ref[:, n * NC:(n + 1) * NC] = (base[n] + r_a[n] + r_b[n]).astype(BF)
    for i in range(1, 8):
        rts(i).wait_send()
    for k in range(nk):
        for j in range(4):
            ag(k, j).wait_send()
        for j in range(3):
            fw(k, j).wait_send()
    for n in range(nn):
        to_sib(n).wait_send()
        send_d(n).wait_send()
        send_a(n).wait_send()
        send_b(n).wait_send()


def _moe(u, h, rt, ws1, ws3, ws2, w1, w3, w2, ny, nx):
    b, d = u.shape
    edev, _, f = w1.shape
    cap = 24
    kc, nk, nn = 512, d // 512, d // NC
    dims = (b, d, f, edev, cap, ny, nx, kc, nk, nn)
    dma = pltpu.SemaphoreType.DMA
    anys = pl.BlockSpec(memory_space=pl.ANY)
    return pl.pallas_call(
        functools.partial(_moe_kernel, dims),
        out_shape=jax.ShapeDtypeStruct((b, d), BF),
        in_specs=[anys] * 9,
        out_specs=pl.BlockSpec(memory_space=pltpu.VMEM),
        scratch_shapes=[
            pltpu.VMEM((nk, 8 * b, kc), BF),
            pltpu.VMEM((8, 16, b), F32),
            pltpu.VMEM((edev * 8 * cap, 2 * f), F32),
            pltpu.VMEM((edev, 8 * cap, f), BF),
            pltpu.VMEM((edev, 8 * cap, kc), BF),
            pltpu.VMEM((4, edev * 2 * cap, 2 * b), BF),
            pltpu.VMEM((4, 6 * b, edev * 2 * cap), BF),
            pltpu.VMEM((NA, kc, 2 * f), BF),
            pltpu.VMEM((NB, f, NC), BF),
            pltpu.VMEM((4, edev * 2 * cap, NC), BF),
            pltpu.VMEM((b, 2 * f), F32),
            pltpu.VMEM((b, f), BF),
            pltpu.VMEM((nn, b, NC), F32),
            pltpu.VMEM((b, d), BF),
            pltpu.VMEM((nn, b, 4 * NC), F32),
            pltpu.VMEM((nn, b, NC), F32),
            pltpu.VMEM((nn, b, NC), F32),
            pltpu.VMEM((nn, b, NC), F32),
            pltpu.VMEM((8 * edev, b), F32),
            pltpu.VMEM((8 * edev, b), F32),
            dma((nk + 2,)), dma((NA, 2)), dma((NB,)),
            dma((nk, 4)), dma((nk, 4)), dma((nk, 3)), dma((nk, 3)), dma((7,)), dma((7,)),
            dma((nn,)), dma((nn,)), dma((nn,)), dma((nn,)), dma((nn,)), dma((nn,)), dma((nn,)), dma((nn,)),
        ],
        compiler_params=pltpu.CompilerParams(collective_id=0, has_side_effects=True, vmem_limit_bytes=67043328),
        name='moe',
    )(u, h, rt, ws1, ws3, ws2, w1, w3, w2)


def solution(mesh):
    ey, ex = mesh.shape['ey'], mesh.shape['ex']
    rows = P(('ey', 'ex'))
    rep = P()

    def local(x, kv_k, kv_v, lens, topk_idx, gates, ln1, ln2, wq, wo, ws1, ws3, ws2, w1, w3, w2):
        h, u = _attn(x, kv_k, kv_v, lens, ln1, ln2, wq, wo)
        pad = ((0, 2), (0, 0))
        rt = jnp.concatenate([jnp.pad(topk_idx.astype(F32).T, pad, constant_values=-1.0), jnp.pad(gates.T, pad)])
        return _moe(u, h, rt, ws1, ws3, ws2, w1, w3, w2, ey, ex)

    return jax.shard_map(
        local, mesh=mesh,
        in_specs=(rows, rows, rows, rows, rows, rows, rep, rep, rep, rep, rep, rep, rep, rows, rows, rows),
        out_specs=rows, check_vma=False)
```

```python
import functools

import jax
import jax.numpy as jnp
from jax import lax
from jax.experimental import pallas as pl
from jax.experimental.pallas import tpu as pltpu
from jax.sharding import PartitionSpec as P

EPS = 1e-6
BF = jnp.bfloat16
F32 = jnp.float32
MESH = pl.DeviceIdType.MESH

NA = 4
NB = 5
NC = 256
UP = 8
UL = 8


def _attn_kernel(dims, lens, x_hbm, ln1, ln2, topk, gates, kk, vv, wq, wo, h_ref, u_ref, rt_ref,
                 kb, vb, wb, q2, o2, xa, xv, shorts, longs, x_sem, k_sem, v_sem, w_sem):
    b, l, dh, hq, d = dims
    sh = 64
    blk = 2 * sh
    cq = d // 4
    top = b * l

    xcopy = pltpu.make_async_copy(x_hbm, xv, x_sem)
    xcopy.start()

    def wcopy(w, i, s):
        return pltpu.make_async_copy(w.at[:, pl.ds(i * cq, cq)], wb.at[:, pl.ds(i * cq, cq)], w_sem.at[s, i])

    for i in range(4):
        wcopy(wq, i, 0).start()

    def srow(i):
        return pl.multiple_of(top - (i // 2 + 1) * blk + lax.rem(i, 2) * sh, sh)

    def kv_s(src, dst, sem, t, i):
        return pltpu.make_async_copy(src.at[t, pl.ds(0, sh)], dst.at[pl.ds(srow(i), sh)], sem.at[0])

    def kv_l(src, dst, sem, t, i):
        return pltpu.make_async_copy(src.at[t], dst.at[pl.ds(pl.multiple_of(i * l, l), l)], sem.at[1])

    def sort_rows(t, c):
        cs, cl = c
        short = lens[t] <= sh
        shorts[cs] = t
        longs[cl] = t

        @pl.when(short)
        def _():
            kv_s(kk, kb, k_sem, t, cs).start()

        @pl.when(jnp.logical_not(short))
        def _():
            kv_l(kk, kb, k_sem, t, cl).start()
        one = short.astype(jnp.int32)
        return cs + one, cl + 1 - one
    ns, nl = lax.fori_loop(0, b, sort_rows, (0, 0))
    odd = lax.rem(ns, 2)

    @pl.when(odd == 1)
    def _():
        kv_s(kk, kb, k_sem, shorts[ns - 1], ns).start()
    last = shorts[jnp.maximum(ns - 1, 0)]
    for j in range(2 * UP):
        shorts[ns + j] = last
    last = longs[jnp.maximum(nl - 1, 0)]
    for j in range(UL):
        longs[nl + j] = last
    ns2 = ns + odd

    def issue_s(i, c):
        kv_s(vv, vb, v_sem, shorts[i], i).start()
        return c
    lax.fori_loop(0, ns2, issue_s, 0)

    def issue_l(i, c):
        kv_l(vv, vb, v_sem, longs[i], i).start()
        return c
    lax.fori_loop(0, nl, issue_l, 0)

    k = topk.shape[0]
    rt_ref[...] = jnp.concatenate(
        [topk[...].astype(F32), jnp.full((8 - k, b), -1.0, F32), gates[...], jnp.zeros((8 - k, b), F32)], axis=0)
    xcopy.wait()
    x = xv[...].astype(F32)
    r = lax.rsqrt(jnp.mean(x * x, axis=-1, keepdims=True) + EPS)
    xa[...] = (x * r * ln1[...].astype(F32).reshape(1, d)).astype(BF)
    for j in range(4):
        wcopy(wq, j, 0).wait()
        q = jnp.dot(xa[...], wb[:, j * cq:(j + 1) * cq], preferred_element_type=F32)
        for hh in range(cq // dh):
            q2[pl.ds(j * (cq // dh) + hh, b, stride=hq), :] = q[:, hh * dh:(hh + 1) * dh].astype(BF).astype(F32)
        wcopy(wo, j, 1).start()

    def wait_s(i, c):
        kv_s(kk, kb, k_sem, 0, 0).wait()
        kv_s(vv, vb, v_sem, 0, 0).wait()
        return c
    lax.fori_loop(0, ns2, wait_s, 0)

    def wait_l(i, c):
        kv_l(kk, kb, k_sem, 0, 0).wait()
        kv_l(vv, vb, v_sem, 0, 0).wait()
        return c
    lax.fori_loop(0, nl, wait_l, 0)

    def qrows(t):
        return pl.ds(pl.multiple_of(t * hq, hq), hq)

    def normal(s):
        e = jnp.exp(s - jnp.max(s, axis=-1, keepdims=True))
        return (e * (1.0 / jnp.sum(e, axis=-1, keepdims=True))).astype(BF)

    nt = (((1,), (1,)), ((), ()))
    pos2 = lax.broadcasted_iota(jnp.int32, (hq, blk), 1)
    scale = dh ** -0.5

    def pairs(it, c):
        ss, idx = [], []
        for j in range(UP):
            i = jnp.minimum(it * UP + j, (ns2 // 2) - 1)
            t0, t1 = shorts[2 * i], shorts[2 * i + 1]
            q = jnp.concatenate([q2[qrows(t0), :], q2[qrows(t1), :]], axis=0).astype(BF)
            kr = pl.ds(pl.multiple_of(top - (i + 1) * blk, blk), blk)
            ss.append(lax.dot_general(q, kb[kr, :], nt, preferred_element_type=F32) * scale)
            idx.append((t0, t1, kr))
        for j in range(UP):
            t0, t1, kr = idx[j]
            s0 = jnp.where(pos2 < lens[t0], ss[j][:hq], -jnp.inf)
            s1 = jnp.where(jnp.logical_and(pos2 >= sh, pos2 < sh + lens[t1]), ss[j][hq:], -jnp.inf)
            o = jnp.dot(normal(jnp.concatenate([s0, s1], axis=0)), vb[kr, :], preferred_element_type=F32)
            o2[qrows(t0), :] = o[:hq]
            o2[qrows(t1), :] = o[hq:]
        return c
    lax.fori_loop(0, (ns2 // 2 + UP - 1) // UP, pairs, 0)

    pos = lax.broadcasted_iota(jnp.int32, (hq, l), 1)

    def single(it, c):
        ss, idx = [], []
        for j in range(UL):
            i = jnp.minimum(it * UL + j, nl - 1)
            t = longs[i]
            kr = pl.ds(pl.multiple_of(i * l, l), l)
            ss.append(lax.dot_general(q2[qrows(t), :].astype(BF), kb[kr, :], nt, preferred_element_type=F32) * scale)
            idx.append((t, kr))
        for j in range(UL):
            t, kr = idx[j]
            p = normal(jnp.where(pos < lens[t], ss[j], -jnp.inf))
            o2[qrows(t), :] = jnp.dot(p, vb[kr, :], preferred_element_type=F32)
        return c
    lax.fori_loop(0, (nl + UL - 1) // UL, single, 0)

    for hh in range(hq):
        xa[:, hh * dh:(hh + 1) * dh] = o2[pl.ds(hh, b, stride=hq), :].astype(BF)
    ssq = jnp.zeros((b, 1), F32)
    for j in range(4):
        cs = slice(j * cq, (j + 1) * cq)
        wcopy(wo, j, 1).wait()
        hv = (xv[:, cs].astype(F32) + jnp.dot(xa[...], wb[:, cs], preferred_element_type=F32)).astype(BF)
        h_ref[:, cs] = hv
        hf = hv.astype(F32)
        ssq += jnp.sum(hf * hf, axis=-1, keepdims=True)
    r = lax.rsqrt(ssq * (1.0 / d) + EPS)
    for j in range(4):
        cs = slice(j * cq, (j + 1) * cq)
        u_ref[:, cs] = (h_ref[:, cs].astype(F32) * r * ln2[cs].astype(F32).reshape(1, cq)).astype(BF)


def _attn(x, kk, vv, lens, ln1, ln2, topk, gates, wq, wo):
    b, d = x.shape
    l, dh = kk.shape[1], kk.shape[3]
    hq = wq.shape[1] // dh
    kk, vv = kk.reshape(b, l, dh), vv.reshape(b, l, dh)
    dma = pltpu.SemaphoreType.DMA
    anys = pl.BlockSpec(memory_space=pl.ANY)
    vm = pl.BlockSpec(memory_space=pltpu.VMEM)
    return pl.pallas_call(
        functools.partial(_attn_kernel, (b, l, dh, hq, d)),
        out_shape=(jax.ShapeDtypeStruct((b, d), BF), jax.ShapeDtypeStruct((b, d), BF),
                   jax.ShapeDtypeStruct((16, b), F32)),
        in_specs=[pl.BlockSpec(memory_space=pltpu.SMEM), anys, vm, vm, vm, vm, anys, anys, anys, anys],
        out_specs=(vm, vm, vm),
        scratch_shapes=[
            pltpu.VMEM((b * l, dh), BF), pltpu.VMEM((b * l, dh), BF), pltpu.VMEM((d, d), BF),
            pltpu.VMEM((b * hq, dh), F32), pltpu.VMEM((b * hq, dh), F32),
            pltpu.VMEM((b, d), BF), pltpu.VMEM((b, d), BF),
            pltpu.SMEM((b + 2 * UP + 2,), jnp.int32), pltpu.SMEM((b + UL + 2,), jnp.int32),
            dma, dma((2,)), dma((2,)), dma((2, 4)),
        ],
        compiler_params=pltpu.CompilerParams(vmem_limit_bytes=67043328),
        name='attn',
    )(lens, x, ln1, ln2, topk.T, gates.T, kk, vv, wq, wo)


def _moe_kernel(dims, u_ref, h_ref, rt_ref, ws1, ws3, ws2, w1, w3, w2, y_ref,
                ug, rt, acc, z, xin, s1h, pg, ring_a, ring_b, fb, acc_s, z_s, base, hv, sib, r_d, r_a, r_b,
                keys, gts, loc_sem, a_sem, b_sem, ag_s, ag_r, fw_s, fw_r, rt_s, rt_r, sb_s, sb_r,
                rd_s, rd_r, ra_s, ra_r, rb_s, rb_r):
    b, d, f, edev, cap, ny, nx, kc, chunks, nn = dims
    nk = len(chunks)
    rows = 8 * cap
    half = 2 * cap
    y = lax.axis_index('ey')
    ex = lax.axis_index('ex')
    x = ex // 2
    c = ex % 2
    me = y * nx + ex
    peers = [(y, 2 * (1 - x) + c), (1 - y, 2 * x + c), (1 - y, 2 * (1 - x) + c), (y, 2 * x + 1 - c)]
    pa = ((1 - c) * y + c * (1 - y), 2 * ((1 - c) * (1 - x) + c * x) + c)
    pb = ((1 - c) * (1 - y) + c * y, 2 * ((1 - c) * x + c * (1 - x)) + c)
    chip = y * 2 + x
    chip_a = pa[0] * 2 + pa[1] // 2
    chip_b = pb[0] * 2 + pb[1] // 2
    chip_d = (1 - y) * 2 + 1 - x
    sibling = peers[3]

    def remote(src, dst, ss, rs, dev):
        return pltpu.make_async_remote_copy(src_ref=src, dst_ref=dst, send_sem=ss, recv_sem=rs,
                                            device_id=dev, device_id_type=MESH)

    def urows(k, dev):
        return ug.at[pl.ds(pl.multiple_of(dev * b, b), b), pl.ds(*chunks[k])]

    def ag(k, j):
        return remote(u_ref.at[:, pl.ds(*chunks[k])], urows(k, me), ag_s.at[k, j], ag_r.at[k, j], peers[j])

    def fw(k, j):
        src = peers[j][0] * nx + peers[j][1]
        return remote(urows(k, src), urows(k, src), fw_s.at[k, j], fw_r.at[k, j], sibling)

    def rts(i):
        t = lax.rem(me + i, 8)
        return remote(rt_ref, rt.at[me], rt_s.at[i - 1], rt_r.at[i - 1], (t // nx, lax.rem(t, nx)))

    def copy_a(slot, start, size, e):
        ks = pl.ds(start, size)
        s1 = ws1.at[ks] if e is None else w1.at[e, ks]
        s3 = ws3.at[ks] if e is None else w3.at[e, ks]
        return (pltpu.make_async_copy(s1, ring_a.at[slot, pl.ds(0, size), pl.ds(0, f)], a_sem.at[slot, 0]),
                pltpu.make_async_copy(s3, ring_a.at[slot, pl.ds(0, size), pl.ds(f, f)], a_sem.at[slot, 1]))

    def shared_a(i):
        start = i * kc if isinstance(i, int) else pl.multiple_of(i * kc, kc)
        return copy_a(i, start, kc, None)

    def copy_b(t, n, e):
        slot = t % NB if isinstance(t, int) else lax.rem(t, NB)
        ns = pl.ds(n * NC if isinstance(n, int) else pl.multiple_of(n * NC, NC), NC)
        src = ws2.at[:, ns] if e is None else w2.at[e, :, ns]
        return pltpu.make_async_copy(src, ring_b.at[slot], b_sem.at[slot])

    for t in range(NA):
        for q in copy_a(t, *chunks[0], t):
            q.start()
    own = pltpu.make_async_copy(u_ref, ug.at[pl.ds(pl.multiple_of(me * b, b), b)], loc_sem.at[0])
    own.start()
    own_h = pltpu.make_async_copy(h_ref, hv, loc_sem.at[1])
    own_h.start()
    own_rt = pltpu.make_async_copy(rt_ref, rt.at[me], loc_sem.at[2])
    own_rt.start()
    for t in range(NB):
        copy_b(t, 0, t).start()

    barrier = pltpu.get_barrier_semaphore()
    for i in range(1, 8):
        t = lax.rem(me + i, 8)
        pl.semaphore_signal(barrier, inc=1, device_id=(t // nx, lax.rem(t, nx)), device_id_type=MESH)
    pl.semaphore_wait(barrier, 7)

    for i in range(1, 8):
        rts(i).start()
    for k in range(nk):
        for j in range(4):
            ag(k, j).start()

    def swiglu(g, v):
        return (g * (1.0 / (1.0 + jnp.exp(-g))) * v).astype(BF)

    own_rt.wait()
    for i in range(1, 8):
        rts(i).wait_recv()
    for s in range(8):
        tk = rt[s, 0:8, :]
        gt = rt[s, 8:16, :]
        for e in range(edev):
            m = tk == (me * edev + e).astype(F32)
            keys[s * edev + e:s * edev + e + 1, :] = jnp.sum(jnp.where(m, 1.0, 0.0), axis=0, keepdims=True)
            gts[s * edev + e:s * edev + e + 1, :] = jnp.sum(jnp.where(m, gt, 0.0), axis=0, keepdims=True)
    chosen = keys[...]
    before = (lax.broadcasted_iota(jnp.int32, (b, b), 0) < lax.broadcasted_iota(jnp.int32, (b, b), 1))
    rank = jnp.dot(chosen.astype(BF), jnp.where(before, 1.0, 0.0).astype(BF), preferred_element_type=F32)
    keys[...] = jnp.where(chosen > 0.0, rank, -1.0)
    slot_no = lax.broadcasted_iota(jnp.int32, (cap, b), 0).astype(F32)
    zero = jnp.zeros((cap, b), F32)
    for p in range(4):
        parts = []
        for e in range(edev):
            i0, i1 = 2 * p * edev + e, (2 * p + 1) * edev + e
            one0 = jnp.where(keys[i0:i0 + 1, :] == slot_no, 1.0, 0.0)
            one1 = jnp.where(keys[i1:i1 + 1, :] == slot_no, 1.0, 0.0)
            s1h[p, e * half:(e + 1) * half, :] = jnp.concatenate(
                [jnp.concatenate([one0, zero], axis=1), jnp.concatenate([zero, one1], axis=1)], axis=0).astype(BF)
            parts.append(jnp.concatenate(
                [jnp.concatenate([one0 * gts[i0:i0 + 1, :], zero], axis=1),
                 jnp.concatenate([zero, one1 * gts[i1:i1 + 1, :]], axis=1)], axis=0))
        g = jnp.concatenate(parts, axis=0).T
        hi = g.astype(BF)
        rest = g - hi.astype(F32)
        mid = rest.astype(BF)
        lo = (rest - mid.astype(F32)).astype(BF)
        pg[p, 0:2 * b, :] = hi
        pg[p, 2 * b:4 * b, :] = mid
        pg[p, 4 * b:6 * b, :] = lo

    def forward(k):
        for j in range(3):
            ag(k, j).wait_recv()
            fw(k, j).start()

    forward(0)
    own.wait()
    for k in range(nk):
        ag(k, 3).wait_recv()
        for j in range(3):
            fw(k, j).wait_recv()
        start, size = chunks[k]
        for p in range(4):
            dsp = jnp.dot(s1h[p], ug[p * 2 * b:(p + 1) * 2 * b, start:start + size],
                          preferred_element_type=F32).astype(BF)
            for e in range(edev):
                xin[e, p * half:(p + 1) * half, 0:size] = dsp[e * half:(e + 1) * half]

        def expert(e, carry, k=k, start=start, size=size, late=False):
            slot = lax.rem(e, NA)
            for q in copy_a(slot, start, size, e):
                q.wait()
            rs = pl.ds(pl.multiple_of(e * rows, rows), rows)
            r = jnp.dot(xin[e, :, 0:size], ring_a[slot, 0:size, :], preferred_element_type=F32)
            if k == 0:
                acc[rs, :] = r
            else:
                acc[rs, :] += r
            if not late:
                nxt = copy_a(slot, start, size, e + NA)
            elif k + 1 < nk:
                nxt = copy_a(slot, *chunks[k + 1], e + NA - edev)
            else:
                nxt = shared_a(slot)
            for q in nxt:
                q.start()
            if k == nk - 1:
                z[e] = swiglu(acc[rs, pl.ds(0, f)], acc[rs, pl.ds(f, f)])
            return carry
        lax.fori_loop(0, edev - NA, expert, 0)
        if k + 1 < nk:
            forward(k + 1)
        lax.fori_loop(edev - NA, edev, functools.partial(expert, late=True), 0)

    def part(n, core, p):
        col = (core * 4 + p) * NC
        col = col if isinstance(col, int) else pl.multiple_of(col, NC)
        return (pl.ds(pl.multiple_of(n * b, b), b), pl.ds(col, NC))

    def to_sib(n):
        src = acc.at[pl.ds(pl.multiple_of(n * b, b), b), pl.ds(pl.multiple_of((1 - c) * 4 * NC, 4 * NC), 4 * NC)]
        return remote(src, sib.at[n], sb_s.at[n], sb_r.at[n], sibling)

    def send_d(n):
        return remote(acc.at[part(n, c, chip_d)], r_d.at[n], rd_s.at[n], rd_r.at[n], pa)

    def send_a(n):
        return remote(acc.at[part(n, c, chip_a)], r_a.at[n], ra_s.at[n], ra_r.at[n], pa)

    def send_b(n):
        return remote(acc.at[part(n, c, chip_b)], r_b.at[n], rb_s.at[n], rb_r.at[n], pb)

    def both(n, p):
        return acc[part(n, c, p)] + sib[n, :, pl.ds(pl.multiple_of(p * NC, NC), NC)]

    def stage1(n):
        to_sib(n).wait_recv()
        acc[part(n, c, chip_d)] = both(n, chip_d)
        send_d(n).start()
        acc[part(n, c, chip_a)] = both(n, chip_a)
        if isinstance(n, int):
            send_a(n - 1).start()
        else:
            @pl.when(n > 0)
            def _():
                send_a(n - 1).start()
        base[n] = both(n, chip)

    def stage2(n):
        send_d(n).wait_recv()
        acc[part(n, c, chip_b)] = both(n, chip_b) + r_d[n]
        send_b(n).start()

    def block(n, carry):
        def down(e, cc):
            i = n * edev + e
            slot = lax.rem(i, NB)
            copy_b(i, n, e).wait()
            r = jnp.dot(z[e], ring_b[slot], preferred_element_type=F32).astype(BF)
            for p in range(4):
                fb[p, pl.ds(pl.multiple_of(e * half, half), half), :] = r[p * half:(p + 1) * half]

            @pl.when(i + NB < nn * edev)
            def _():
                i2 = i + NB
                copy_b(i2, i2 // edev, lax.rem(i2, edev)).start()

            @pl.when(i + NB >= nn * edev)
            def _():
                copy_b(i + NB, i + NB - nn * edev, None).start()
            return cc
        lax.fori_loop(0, edev // 2, down, 0)

        @pl.when(n > 0)
        def _():
            stage1(n - 1)
        lax.fori_loop(edev // 2, edev, down, 0)
        for p in range(4):
            q = jnp.dot(pg[p], fb[p], preferred_element_type=F32)
            q = q[0:2 * b] + q[2 * b:4 * b] + q[4 * b:6 * b]
            for core in range(2):
                acc[part(n, core, p)] = q[core * b:(core + 1) * b]
        to_sib(n).start()

        @pl.when(n > 1)
        def _():
            stage2(n - 2)
        return carry
    lax.fori_loop(0, nn, block, 0)
    stage1(nn - 1)
    send_a(nn - 1).start()
    stage2(nn - 2)

    for i in range(d // kc):
        for q in shared_a(i):
            q.wait()
        r = jnp.dot(ug[pl.ds(pl.multiple_of(me * b, b), b), i * kc:(i + 1) * kc], ring_a[i],
                    preferred_element_type=F32)
        if i == 0:
            acc_s[...] = r
        else:
            acc_s[...] += r
    z_s[...] = swiglu(acc_s[:, :f], acc_s[:, f:])
    stage2(nn - 1)
    own_h.wait()
    for n in range(nn):
        t = nn * edev + n
        copy_b(t, n, None).wait()
        sh = jnp.dot(z_s[...], ring_b[t % NB], preferred_element_type=F32).astype(BF).astype(F32)
        base[n] += hv[:, n * NC:(n + 1) * NC].astype(F32) + sh
        if n + NB < nn:
            copy_b(t + NB, n + NB, None).start()
    for n in range(nn):
        send_a(n).wait_recv()
        send_b(n).wait_recv()
        y_ref[:, n * NC:(n + 1) * NC] = (base[n] + r_a[n] + r_b[n]).astype(BF)
    for i in range(1, 8):
        rts(i).wait_send()
    for k in range(nk):
        for j in range(4):
            ag(k, j).wait_send()
        for j in range(3):
            fw(k, j).wait_send()
    for n in range(nn):
        to_sib(n).wait_send()
        send_d(n).wait_send()
        send_a(n).wait_send()
        send_b(n).wait_send()


def _moe(u, h, rt, ws1, ws3, ws2, w1, w3, w2, ny, nx):
    b, d = u.shape
    edev, _, f = w1.shape
    cap = 24
    kc, nn = 512, d // NC
    chunks = ((0, 256), (256, 256), (512, 512), (1024, 512), (1536, 512))
    nk = len(chunks)
    dims = (b, d, f, edev, cap, ny, nx, kc, chunks, nn)
    dma = pltpu.SemaphoreType.DMA
    anys = pl.BlockSpec(memory_space=pl.ANY)
    return pl.pallas_call(
        functools.partial(_moe_kernel, dims),
        out_shape=jax.ShapeDtypeStruct((b, d), BF),
        in_specs=[anys] * 9,
        out_specs=pl.BlockSpec(memory_space=pltpu.VMEM),
        scratch_shapes=[
            pltpu.VMEM((8 * b, d), BF),
            pltpu.VMEM((8, 16, b), F32),
            pltpu.VMEM((edev * 8 * cap, 2 * f), F32),
            pltpu.VMEM((edev, 8 * cap, f), BF),
            pltpu.VMEM((edev, 8 * cap, kc), BF),
            pltpu.VMEM((4, edev * 2 * cap, 2 * b), BF),
            pltpu.VMEM((4, 6 * b, edev * 2 * cap), BF),
            pltpu.VMEM((NA, kc, 2 * f), BF),
            pltpu.VMEM((NB, f, NC), BF),
            pltpu.VMEM((4, edev * 2 * cap, NC), BF),
            pltpu.VMEM((b, 2 * f), F32),
            pltpu.VMEM((b, f), BF),
            pltpu.VMEM((nn, b, NC), F32),
            pltpu.VMEM((b, d), BF),
            pltpu.VMEM((nn, b, 4 * NC), F32),
            pltpu.VMEM((nn, b, NC), F32),
            pltpu.VMEM((nn, b, NC), F32),
            pltpu.VMEM((nn, b, NC), F32),
            pltpu.VMEM((8 * edev, b), F32),
            pltpu.VMEM((8 * edev, b), F32),
            dma((3,)), dma((NA, 2)), dma((NB,)),
            dma((nk, 4)), dma((nk, 4)), dma((nk, 3)), dma((nk, 3)), dma((7,)), dma((7,)),
            dma((nn,)), dma((nn,)), dma((nn,)), dma((nn,)), dma((nn,)), dma((nn,)), dma((nn,)), dma((nn,)),
        ],
        compiler_params=pltpu.CompilerParams(collective_id=0, has_side_effects=True, vmem_limit_bytes=67043328),
        name='moe',
    )(u, h, rt, ws1, ws3, ws2, w1, w3, w2)


def solution(mesh):
    ey, ex = mesh.shape['ey'], mesh.shape['ex']
    rows = P(('ey', 'ex'))
    rep = P()

    def local(x, kv_k, kv_v, lens, topk_idx, gates, ln1, ln2, wq, wo, ws1, ws3, ws2, w1, w3, w2):
        h, u, rt = _attn(x, kv_k, kv_v, lens, ln1, ln2, topk_idx, gates, wq, wo)
        return _moe(u, h, rt, ws1, ws3, ws2, w1, w3, w2, ey, ex)

    return jax.shard_map(
        local, mesh=mesh,
        in_specs=(rows, rows, rows, rows, rows, rows, rep, rep, rep, rep, rep, rep, rep, rows, rows, rows),
        out_specs=rows, check_vma=False)
```

```python
import functools

import jax
import jax.numpy as jnp
from jax import lax
from jax.experimental import pallas as pl
from jax.experimental.pallas import tpu as pltpu
from jax.sharding import PartitionSpec as P

EPS = 1e-6
BF = jnp.bfloat16
F32 = jnp.float32
MESH = pl.DeviceIdType.MESH

NA = 4
NB = 8
ND = 4
NC = 256
UP = 24
UL = 24


def _attn_kernel(dims, lens, x_hbm, ln1, ln2, topk, gates, kk, vv, wq, wo, h_ref, u_ref, rt_ref,
                 kb, vb, wb, q2, o2, xa, xv, shorts, longs, x_sem, kv_sem, w_sem):
    b, l, dh, hq, d = dims
    sh = 64
    blk = 2 * sh
    cq = d // 4
    top = b * l

    xcopy = pltpu.make_async_copy(x_hbm, xv, x_sem)
    xcopy.start()

    def wcopy(w, i, s):
        return pltpu.make_async_copy(w.at[:, pl.ds(i * cq, cq)], wb.at[:, pl.ds(i * cq, cq)], w_sem.at[s, i])

    for i in range(4):
        wcopy(wq, i, 0).start()

    def srow(i):
        return pl.multiple_of(top - (i // 2 + 1) * blk + lax.rem(i, 2) * sh, sh)

    def kv_s(t, i):
        for q, (src, dst) in enumerate(((kk, kb), (vv, vb))):
            pltpu.make_async_copy(src.at[t, pl.ds(0, sh)], dst.at[pl.ds(srow(i), sh)], kv_sem.at[0, q]).start()

    def kv_l(t, i):
        for q, (src, dst) in enumerate(((kk, kb), (vv, vb))):
            pltpu.make_async_copy(src.at[t], dst.at[pl.ds(pl.multiple_of(i * l, l), l)], kv_sem.at[1, q]).start()

    def kv_wait(kind, n_rows):
        r = pl.ds(0, pl.multiple_of(n_rows, sh))
        for q, buf in enumerate((kb, vb)):
            pltpu.make_async_copy(buf.at[r], buf.at[r], kv_sem.at[kind, q]).wait()

    def sort_rows(t, c):
        cs, cl = c
        short = lens[t] <= sh
        shorts[cs] = t
        longs[cl] = t

        @pl.when(short)
        def _():
            kv_s(t, cs)

        @pl.when(jnp.logical_not(short))
        def _():
            kv_l(t, cl)
        one = short.astype(jnp.int32)
        return cs + one, cl + 1 - one
    ns, nl = lax.fori_loop(0, b, sort_rows, (0, 0))
    odd = lax.rem(ns, 2)

    @pl.when(odd == 1)
    def _():
        kv_s(shorts[ns - 1], ns)
    last = shorts[jnp.maximum(ns - 1, 0)]
    shorts[ns] = last
    ns2 = ns + odd

    k = topk.shape[0]
    rt_ref[...] = jnp.concatenate(
        [topk[...].astype(F32), jnp.full((8 - k, b), -1.0, F32), gates[...], jnp.zeros((8 - k, b), F32)], axis=0)
    xcopy.wait()
    x = xv[...].astype(F32)
    r = lax.rsqrt(jnp.mean(x * x, axis=-1, keepdims=True) + EPS)
    xa[...] = (x * r * ln1[...].astype(F32).reshape(1, d)).astype(BF)
    for j in range(4):
        wcopy(wq, j, 0).wait()
        q = jnp.dot(xa[...], wb[:, j * cq:(j + 1) * cq], preferred_element_type=F32)
        for hh in range(cq // dh):
            q2[pl.ds(j * (cq // dh) + hh, b, stride=hq), :] = q[:, hh * dh:(hh + 1) * dh].astype(BF).astype(F32)
        wcopy(wo, j, 1).start()

    def qrows(t):
        return pl.ds(pl.multiple_of(t * hq, hq), hq)

    def normal(s):
        e = jnp.exp(s - jnp.max(s, axis=-1, keepdims=True))
        return (e * (1.0 / jnp.sum(e, axis=-1, keepdims=True))).astype(BF)

    nt = (((1,), (1,)), ((), ()))
    pos2 = lax.broadcasted_iota(jnp.int32, (hq, blk), 1)
    scale = dh ** -0.5

    def pairs(it, c):
        ss, idx = [], []
        for j in range(UP):
            i = jnp.minimum(it * UP + j, (ns2 // 2) - 1)
            t0, t1 = shorts[2 * i], shorts[2 * i + 1]
            q = jnp.concatenate([q2[qrows(t0), :], q2[qrows(t1), :]], axis=0).astype(BF)
            kr = pl.ds(pl.multiple_of(top - (i + 1) * blk, blk), blk)
            ss.append(lax.dot_general(q, kb[kr, :], nt, preferred_element_type=F32) * scale)
            idx.append((t0, t1, kr))
        for j in range(UP):
            t0, t1, kr = idx[j]
            s0 = jnp.where(pos2 < lens[t0], ss[j][:hq], -jnp.inf)
            s1 = jnp.where(jnp.logical_and(pos2 >= sh, pos2 < sh + lens[t1]), ss[j][hq:], -jnp.inf)
            o = jnp.dot(normal(jnp.concatenate([s0, s1], axis=0)), vb[kr, :], preferred_element_type=F32)
            o2[qrows(t0), :] = o[:hq]
            o2[qrows(t1), :] = o[hq:]
        return c
    kv_wait(0, ns2 * sh)
    lax.fori_loop(0, (ns2 // 2 + UP - 1) // UP, pairs, 0)

    pos = lax.broadcasted_iota(jnp.int32, (hq, l), 1)

    def single(it, c):
        ss, idx = [], []
        for j in range(UL):
            i = jnp.minimum(it * UL + j, nl - 1)
            t = longs[i]
            kr = pl.ds(pl.multiple_of(i * l, l), l)
            ss.append(lax.dot_general(q2[qrows(t), :].astype(BF), kb[kr, :], nt, preferred_element_type=F32) * scale)
            idx.append((t, kr))
        for j in range(UL):
            t, kr = idx[j]
            p = normal(jnp.where(pos < lens[t], ss[j], -jnp.inf))
            o2[qrows(t), :] = jnp.dot(p, vb[kr, :], preferred_element_type=F32)
        return c
    kv_wait(1, nl * l)
    lax.fori_loop(0, (nl + UL - 1) // UL, single, 0)

    for hh in range(hq):
        xa[:, hh * dh:(hh + 1) * dh] = o2[pl.ds(hh, b, stride=hq), :].astype(BF)
    ssq = jnp.zeros((b, 1), F32)
    for j in range(4):
        cs = slice(j * cq, (j + 1) * cq)
        wcopy(wo, j, 1).wait()
        hv = (xv[:, cs].astype(F32) + jnp.dot(xa[...], wb[:, cs], preferred_element_type=F32)).astype(BF)
        h_ref[:, cs] = hv
        hf = hv.astype(F32)
        ssq += jnp.sum(hf * hf, axis=-1, keepdims=True)
    r = lax.rsqrt(ssq * (1.0 / d) + EPS)
    for j in range(4):
        cs = slice(j * cq, (j + 1) * cq)
        u_ref[:, cs] = (h_ref[:, cs].astype(F32) * r * ln2[cs].astype(F32).reshape(1, cq)).astype(BF)


def _attn(x, kk, vv, lens, ln1, ln2, topk, gates, wq, wo):
    b, d = x.shape
    l, dh = kk.shape[1], kk.shape[3]
    hq = wq.shape[1] // dh
    kk, vv = kk.reshape(b, l, dh), vv.reshape(b, l, dh)
    dma = pltpu.SemaphoreType.DMA
    anys = pl.BlockSpec(memory_space=pl.ANY)
    vm = pl.BlockSpec(memory_space=pltpu.VMEM)
    return pl.pallas_call(
        functools.partial(_attn_kernel, (b, l, dh, hq, d)),
        out_shape=(jax.ShapeDtypeStruct((b, d), BF), jax.ShapeDtypeStruct((b, d), BF),
                   jax.ShapeDtypeStruct((16, b), F32)),
        in_specs=[pl.BlockSpec(memory_space=pltpu.SMEM), anys, vm, vm, vm, vm, anys, anys, anys, anys],
        out_specs=(vm, vm, vm),
        scratch_shapes=[
            pltpu.VMEM((b * l, dh), BF), pltpu.VMEM((b * l, dh), BF), pltpu.VMEM((d, d), BF),
            pltpu.VMEM((b * hq, dh), F32), pltpu.VMEM((b * hq, dh), F32),
            pltpu.VMEM((b, d), BF), pltpu.VMEM((b, d), BF),
            pltpu.SMEM((b + 2,), jnp.int32), pltpu.SMEM((b + 2,), jnp.int32),
            dma, dma((2, 2)), dma((2, 4)),
        ],
        compiler_params=pltpu.CompilerParams(vmem_limit_bytes=67043328),
        name='attn',
    )(lens, x, ln1, ln2, topk.T, gates.T, kk, vv, wq, wo)


def _moe_kernel(dims, u_ref, h_ref, rt_ref, ws1, ws3, ws2, w1, w3, w2, y_ref,
                ug, rt, acc, z, xin, s1h, pg, ring_a, ring_b, fb, acc_s, z_s, base, hv, sib, r_d, r_a, r_b,
                keys, gts, loc_sem, a_sem, b_sem, ag_s, ag_r, fw_s, fw_r, rt_s, rt_r, sb_s, sb_r,
                rd_s, rd_r, ra_s, ra_r, rb_s, rb_r):
    b, d, f, edev, cap, ny, nx, kc, chunks, nn = dims
    nk = len(chunks)
    rows = 8 * cap
    half = 2 * cap
    y = lax.axis_index('ey')
    ex = lax.axis_index('ex')
    x = ex // 2
    c = ex % 2
    me = y * nx + ex
    peers = [(y, 2 * (1 - x) + c), (1 - y, 2 * x + c), (1 - y, 2 * (1 - x) + c), (y, 2 * x + 1 - c)]
    pa = ((1 - c) * y + c * (1 - y), 2 * ((1 - c) * (1 - x) + c * x) + c)
    pb = ((1 - c) * (1 - y) + c * y, 2 * ((1 - c) * x + c * (1 - x)) + c)
    chip = y * 2 + x
    chip_a = pa[0] * 2 + pa[1] // 2
    chip_b = pb[0] * 2 + pb[1] // 2
    chip_d = (1 - y) * 2 + 1 - x
    sibling = peers[3]

    def remote(src, dst, ss, rs, dev):
        return pltpu.make_async_remote_copy(src_ref=src, dst_ref=dst, send_sem=ss, recv_sem=rs,
                                            device_id=dev, device_id_type=MESH)

    def urows(k, dev):
        return ug.at[pl.ds(pl.multiple_of(dev * b, b), b), pl.ds(*chunks[k])]

    def ag(k, j):
        return remote(u_ref.at[:, pl.ds(*chunks[k])], urows(k, me), ag_s.at[k, j], ag_r.at[k, j], peers[j])

    def fw(k, j):
        src = peers[j][0] * nx + peers[j][1]
        return remote(urows(k, src), urows(k, src), fw_s.at[k, j], fw_r.at[k, j], sibling)

    def rts(i):
        t = lax.rem(me + i, 8)
        return remote(rt_ref, rt.at[me], rt_s.at[i - 1], rt_r.at[i - 1], (t // nx, lax.rem(t, nx)))

    def copy_a(slot, start, size, e):
        ks = pl.ds(start, size)
        s1 = ws1.at[ks] if e is None else w1.at[e, ks]
        s3 = ws3.at[ks] if e is None else w3.at[e, ks]
        return (pltpu.make_async_copy(s1, ring_a.at[slot, pl.ds(0, size), pl.ds(0, f)], a_sem.at[slot, 0]),
                pltpu.make_async_copy(s3, ring_a.at[slot, pl.ds(0, size), pl.ds(f, f)], a_sem.at[slot, 1]))

    def shared_a(i):
        start = i * kc if isinstance(i, int) else pl.multiple_of(i * kc, kc)
        return copy_a(i, start, kc, None)

    def copy_b(t, n, e):
        slot = t % NB if isinstance(t, int) else lax.rem(t, NB)
        ns = pl.ds(n * NC if isinstance(n, int) else pl.multiple_of(n * NC, NC), NC)
        src = ws2.at[:, ns] if e is None else w2.at[e, :, ns]
        return pltpu.make_async_copy(src, ring_b.at[slot], b_sem.at[slot])

    for t in range(NA):
        for q in copy_a(t, *chunks[0], t):
            q.start()
    own = pltpu.make_async_copy(u_ref, ug.at[pl.ds(pl.multiple_of(me * b, b), b)], loc_sem.at[0])
    own.start()
    own_h = pltpu.make_async_copy(h_ref, hv, loc_sem.at[1])
    own_h.start()
    own_rt = pltpu.make_async_copy(rt_ref, rt.at[me], loc_sem.at[2])
    own_rt.start()
    for t in range(NB):
        copy_b(t, 0, t).start()

    barrier = pltpu.get_barrier_semaphore()
    for i in range(1, 8):
        t = lax.rem(me + i, 8)
        pl.semaphore_signal(barrier, inc=1, device_id=(t // nx, lax.rem(t, nx)), device_id_type=MESH)
    pl.semaphore_wait(barrier, 7)

    for i in range(1, 8):
        rts(i).start()
    for k in range(nk):
        for j in range(4):
            ag(k, j).start()

    def swiglu(g, v):
        return (g * (1.0 / (1.0 + jnp.exp(-g))) * v).astype(BF)

    own_rt.wait()
    for i in range(1, 8):
        rts(i).wait_recv()
    for s in range(8):
        tk = rt[s, 0:8, :]
        gt = rt[s, 8:16, :]
        for e in range(edev):
            m = tk == (me * edev + e).astype(F32)
            keys[s * edev + e:s * edev + e + 1, :] = jnp.sum(jnp.where(m, 1.0, 0.0), axis=0, keepdims=True)
            gts[s * edev + e:s * edev + e + 1, :] = jnp.sum(jnp.where(m, gt, 0.0), axis=0, keepdims=True)
    chosen = keys[...]
    before = (lax.broadcasted_iota(jnp.int32, (b, b), 0) < lax.broadcasted_iota(jnp.int32, (b, b), 1))
    rank = jnp.dot(chosen.astype(BF), jnp.where(before, 1.0, 0.0).astype(BF), preferred_element_type=F32)
    keys[...] = jnp.where(chosen > 0.0, rank, -1.0)
    slot_no = lax.broadcasted_iota(jnp.int32, (cap, b), 0).astype(F32)
    zero = jnp.zeros((cap, b), F32)
    for p in range(4):
        parts = []
        for e in range(edev):
            i0, i1 = 2 * p * edev + e, (2 * p + 1) * edev + e
            one0 = jnp.where(keys[i0:i0 + 1, :] == slot_no, 1.0, 0.0)
            one1 = jnp.where(keys[i1:i1 + 1, :] == slot_no, 1.0, 0.0)
            s1h[p, e * half:(e + 1) * half, :] = jnp.concatenate(
                [jnp.concatenate([one0, zero], axis=1), jnp.concatenate([zero, one1], axis=1)], axis=0).astype(BF)
            parts.append(jnp.concatenate(
                [jnp.concatenate([one0 * gts[i0:i0 + 1, :], zero], axis=1),
                 jnp.concatenate([zero, one1 * gts[i1:i1 + 1, :]], axis=1)], axis=0))
        g = jnp.concatenate(parts, axis=0).T
        hi = g.astype(BF)
        rest = g - hi.astype(F32)
        mid = rest.astype(BF)
        lo = (rest - mid.astype(F32)).astype(BF)
        pg[p, 0:2 * b, :] = hi
        pg[p, 2 * b:4 * b, :] = mid
        pg[p, 4 * b:6 * b, :] = lo

    def forward(k):
        for j in range(3):
            ag(k, j).wait_recv()
            fw(k, j).start()

    forward(0)
    own.wait()
    for k in range(nk):
        ag(k, 3).wait_recv()
        for j in range(3):
            fw(k, j).wait_recv()
        start, size = chunks[k]
        for p in range(4):
            dsp = jnp.dot(s1h[p], ug[p * 2 * b:(p + 1) * 2 * b, start:start + size],
                          preferred_element_type=F32).astype(BF)
            for e in range(edev):
                xin[e, p * half:(p + 1) * half, 0:size] = dsp[e * half:(e + 1) * half]

        def expert(e, carry, k=k, start=start, size=size, late=False):
            slot = lax.rem(e, NA)
            for q in copy_a(slot, start, size, e):
                q.wait()
            rs = pl.ds(pl.multiple_of(e * rows, rows), rows)
            r = jnp.dot(xin[e, :, 0:size], ring_a[slot, 0:size, :], preferred_element_type=F32)
            if k == 0:
                acc[rs, :] = r
            else:
                acc[rs, :] += r
            if not late:
                nxt = copy_a(slot, start, size, e + NA)
            elif k + 1 < nk:
                nxt = copy_a(slot, *chunks[k + 1], e + NA - edev)
            else:
                nxt = shared_a(slot)
            for q in nxt:
                q.start()
            if k == nk - 1:
                z[e] = swiglu(acc[rs, pl.ds(0, f)], acc[rs, pl.ds(f, f)])
            return carry
        lax.fori_loop(0, edev - NA, expert, 0)
        if k + 1 < nk:
            forward(k + 1)
        lax.fori_loop(edev - NA, edev, functools.partial(expert, late=True), 0)

    def part(n, core, p):
        col = (core * 4 + p) * NC
        col = col if isinstance(col, int) else pl.multiple_of(col, NC)
        return (pl.ds(pl.multiple_of(n * b, b), b), pl.ds(col, NC))

    def to_sib(n):
        src = acc.at[pl.ds(pl.multiple_of(n * b, b), b), pl.ds(pl.multiple_of((1 - c) * 4 * NC, 4 * NC), 4 * NC)]
        return remote(src, sib.at[n], sb_s.at[n], sb_r.at[n], sibling)

    def send_d(n):
        return remote(acc.at[part(n, c, chip_d)], r_d.at[n], rd_s.at[n], rd_r.at[n], pa)

    def send_a(n):
        return remote(acc.at[part(n, c, chip_a)], r_a.at[n], ra_s.at[n], ra_r.at[n], pa)

    def send_b(n):
        return remote(acc.at[part(n, c, chip_b)], r_b.at[n], rb_s.at[n], rb_r.at[n], pb)

    def both(n, p):
        return acc[part(n, c, p)] + sib[n, :, pl.ds(pl.multiple_of(p * NC, NC), NC)]

    def stage1(n):
        to_sib(n).wait_recv()
        acc[part(n, c, chip_d)] = both(n, chip_d)
        send_d(n).start()
        acc[part(n, c, chip_a)] = both(n, chip_a)
        send_a(n).start()
        base[n] = both(n, chip)

    def stage2(n):
        send_d(n).wait_recv()
        acc[part(n, c, chip_b)] = both(n, chip_b) + r_d[n]
        send_b(n).start()

    def block(n, carry):
        def down(e2, cc):
            es = [e2 * ND + j for j in range(ND)]
            for e in es:
                copy_b(n * edev + e, n, e).wait()
            rs = [jnp.dot(z[e], ring_b[lax.rem(n * edev + e, NB)], preferred_element_type=F32).astype(BF) for e in es]
            for e, r in zip(es, rs):
                for p in range(4):
                    fb[p, pl.ds(pl.multiple_of(e * half, half), half), :] = r[p * half:(p + 1) * half]
            for e in es:
                i2 = n * edev + e + NB

                @pl.when(i2 < nn * edev)
                def _():
                    copy_b(i2, i2 // edev, lax.rem(i2, edev)).start()

                @pl.when(i2 >= nn * edev)
                def _():
                    copy_b(i2, i2 - nn * edev, None).start()
            return cc
        lax.fori_loop(0, edev // 2 // ND, down, 0)

        @pl.when(n > 0)
        def _():
            stage1(n - 1)
        lax.fori_loop(edev // 2 // ND, edev // ND, down, 0)
        for p in range(4):
            q = jnp.dot(pg[p], fb[p], preferred_element_type=F32)
            q = q[0:2 * b] + q[2 * b:4 * b] + q[4 * b:6 * b]
            for core in range(2):
                acc[part(n, core, p)] = q[core * b:(core + 1) * b]
        to_sib(n).start()

        @pl.when(n > 1)
        def _():
            stage2(n - 2)

        @pl.when(n == nn // 2)
        def _():
            pass
        return carry
    lax.fori_loop(0, nn, block, 0)
    stage1(nn - 1)
    stage2(nn - 2)

    for i in range(d // kc):
        for q in shared_a(i):
            q.wait()
        r = jnp.dot(ug[pl.ds(pl.multiple_of(me * b, b), b), i * kc:(i + 1) * kc], ring_a[i],
                    preferred_element_type=F32)
        if i == 0:
            acc_s[...] = r
        else:
            acc_s[...] += r
    z_s[...] = swiglu(acc_s[:, :f], acc_s[:, f:])
    stage2(nn - 1)
    own_h.wait()
    for n in range(nn):
        t = nn * edev + n
        copy_b(t, n, None).wait()
        sh = jnp.dot(z_s[...], ring_b[t % NB], preferred_element_type=F32).astype(BF).astype(F32)
        base[n] += hv[:, n * NC:(n + 1) * NC].astype(F32) + sh
        if n + NB < nn:
            copy_b(t + NB, n + NB, None).start()
    for n in range(nn):
        send_a(n).wait_recv()
        send_b(n).wait_recv()
        y_ref[:, n * NC:(n + 1) * NC] = (base[n] + r_a[n] + r_b[n]).astype(BF)
    for i in range(1, 8):
        rts(i).wait_send()
    for k in range(nk):
        for j in range(4):
            ag(k, j).wait_send()
        for j in range(3):
            fw(k, j).wait_send()
    for n in range(nn):
        to_sib(n).wait_send()
        send_d(n).wait_send()
        send_a(n).wait_send()
        send_b(n).wait_send()


def _moe(u, h, rt, ws1, ws3, ws2, w1, w3, w2, ny, nx):
    b, d = u.shape
    edev, _, f = w1.shape
    cap = 24
    kc, nn = 512, d // NC
    chunks = ((0, 256), (256, 256), (512, 512), (1024, 512), (1536, 512))
    nk = len(chunks)
    dims = (b, d, f, edev, cap, ny, nx, kc, chunks, nn)
    dma = pltpu.SemaphoreType.DMA
    anys = pl.BlockSpec(memory_space=pl.ANY)
    return pl.pallas_call(
        functools.partial(_moe_kernel, dims),
        out_shape=jax.ShapeDtypeStruct((b, d), BF),
        in_specs=[anys] * 9,
        out_specs=pl.BlockSpec(memory_space=pltpu.VMEM),
        scratch_shapes=[
            pltpu.VMEM((8 * b, d), BF),
            pltpu.VMEM((8, 16, b), F32),
            pltpu.VMEM((edev * 8 * cap, 2 * f), F32),
            pltpu.VMEM((edev, 8 * cap, f), BF),
            pltpu.VMEM((edev, 8 * cap, kc), BF),
            pltpu.VMEM((4, edev * 2 * cap, 2 * b), BF),
            pltpu.VMEM((4, 6 * b, edev * 2 * cap), BF),
            pltpu.VMEM((NA, kc, 2 * f), BF),
            pltpu.VMEM((NB, f, NC), BF),
            pltpu.VMEM((4, edev * 2 * cap, NC), BF),
            pltpu.VMEM((b, 2 * f), F32),
            pltpu.VMEM((b, f), BF),
            pltpu.VMEM((nn, b, NC), F32),
            pltpu.VMEM((b, d), BF),
            pltpu.VMEM((nn, b, 4 * NC), F32),
            pltpu.VMEM((nn, b, NC), F32),
            pltpu.VMEM((nn, b, NC), F32),
            pltpu.VMEM((nn, b, NC), F32),
            pltpu.VMEM((8 * edev, b), F32),
            pltpu.VMEM((8 * edev, b), F32),
            dma((3,)), dma((NA, 2)), dma((NB,)),
            dma((nk, 4)), dma((nk, 4)), dma((nk, 3)), dma((nk, 3)), dma((7,)), dma((7,)),
            dma((nn,)), dma((nn,)), dma((nn,)), dma((nn,)), dma((nn,)), dma((nn,)), dma((nn,)), dma((nn,)),
        ],
        compiler_params=pltpu.CompilerParams(collective_id=0, has_side_effects=True, vmem_limit_bytes=67043328),
        name='moe',
    )(u, h, rt, ws1, ws3, ws2, w1, w3, w2)


def solution(mesh):
    ey, ex = mesh.shape['ey'], mesh.shape['ex']
    rows = P(('ey', 'ex'))
    rep = P()

    def local(x, kv_k, kv_v, lens, topk_idx, gates, ln1, ln2, wq, wo, ws1, ws3, ws2, w1, w3, w2):
        h, u, rt = _attn(x, kv_k, kv_v, lens, ln1, ln2, topk_idx, gates, wq, wo)
        return _moe(u, h, rt, ws1, ws3, ws2, w1, w3, w2, ey, ex)

    return jax.shard_map(
        local, mesh=mesh,
        in_specs=(rows, rows, rows, rows, rows, rows, rep, rep, rep, rep, rep, rep, rep, rows, rows, rows),
        out_specs=rows, check_vma=False)
```

```python
import functools

import jax
import jax.numpy as jnp
from jax import lax
from jax.experimental import pallas as pl
from jax.experimental.pallas import tpu as pltpu
from jax.sharding import PartitionSpec as P

EPS = 1e-6
BF = jnp.bfloat16
F32 = jnp.float32
MESH = pl.DeviceIdType.MESH

NA = 4
NB = 8
ND = 4
NC = 256
UP = 24
UL = 24


def _attn_kernel(dims, lens, x_hbm, ln1, ln2, topk, gates, kk, vv, wq, wo, h_hbm, u_hbm, rt_ref,
                 h_ref, u_ref, out_sem, kb, vb, wb, q2, o2, xa, xv, shorts, longs, x_sem, kv_sem, w_sem):
    b, l, dh, hq, d = dims
    sh = 64
    blk = 2 * sh
    cq = d // 4
    top = b * l

    xcopy = pltpu.make_async_copy(x_hbm, xv, x_sem)
    xcopy.start()

    def wcopy(w, i, s):
        return pltpu.make_async_copy(w.at[:, pl.ds(i * cq, cq)], wb.at[:, pl.ds(i * cq, cq)], w_sem.at[s, i])

    for i in range(4):
        wcopy(wq, i, 0).start()

    def srow(i):
        return pl.multiple_of(top - (i // 2 + 1) * blk + lax.rem(i, 2) * sh, sh)

    def kv_s(t, i):
        for q, (src, dst) in enumerate(((kk, kb), (vv, vb))):
            pltpu.make_async_copy(src.at[t, pl.ds(0, sh)], dst.at[pl.ds(srow(i), sh)], kv_sem.at[0, q]).start()

    def kv_l(t, i):
        for q, (src, dst) in enumerate(((kk, kb), (vv, vb))):
            pltpu.make_async_copy(src.at[t], dst.at[pl.ds(pl.multiple_of(i * l, l), l)], kv_sem.at[1, q]).start()

    def kv_wait(kind, n_rows):
        r = pl.ds(0, pl.multiple_of(n_rows, sh))
        for q, buf in enumerate((kb, vb)):
            pltpu.make_async_copy(buf.at[r], buf.at[r], kv_sem.at[kind, q]).wait()

    def sort_rows(t, c):
        cs, cl = c
        short = lens[t] <= sh
        shorts[cs] = t
        longs[cl] = t
        one = (lens[t] <= sh).astype(jnp.int32)
        return cs + one, cl + 1 - one
    ns, nl = lax.fori_loop(0, b, sort_rows, (0, 0), unroll=4)
    last = shorts[jnp.maximum(ns - 1, 0)]
    shorts[ns] = last
    ns2 = ns + lax.rem(ns, 2)

    def issue_s(i, carry):
        kv_s(shorts[i], i)
        return carry
    lax.fori_loop(0, ns2, issue_s, 0)

    def issue_l(i, carry):
        kv_l(longs[i], i)
        return carry
    lax.fori_loop(0, nl, issue_l, 0)

    k = topk.shape[0]
    rt_ref[...] = jnp.concatenate(
        [topk[...].astype(F32), jnp.full((8 - k, b), -1.0, F32), gates[...], jnp.zeros((8 - k, b), F32)], axis=0)
    xcopy.wait()
    x = xv[...].astype(F32)
    r = lax.rsqrt(jnp.mean(x * x, axis=-1, keepdims=True) + EPS)
    xa[...] = (x * r * ln1[...].astype(F32).reshape(1, d)).astype(BF)
    for j in range(4):
        wcopy(wq, j, 0).wait()
        q = jnp.dot(xa[...], wb[:, j * cq:(j + 1) * cq], preferred_element_type=F32)
        for hh in range(cq // dh):
            q2[pl.ds(j * (cq // dh) + hh, b, stride=hq), :] = q[:, hh * dh:(hh + 1) * dh].astype(BF).astype(F32)
        wcopy(wo, j, 1).start()

    def qrows(t):
        return pl.ds(pl.multiple_of(t * hq, hq), hq)

    def normal(s):
        e = jnp.exp(s - jnp.max(s, axis=-1, keepdims=True))
        return (e * (1.0 / jnp.sum(e, axis=-1, keepdims=True))).astype(BF)

    nt = (((1,), (1,)), ((), ()))
    pos2 = lax.broadcasted_iota(jnp.int32, (hq, blk), 1)
    scale = dh ** -0.5

    def pairs(it, c):
        ss, idx = [], []
        for j in range(UP):
            i = jnp.minimum(it * UP + j, (ns2 // 2) - 1)
            t0, t1 = shorts[2 * i], shorts[2 * i + 1]
            q = jnp.concatenate([q2[qrows(t0), :], q2[qrows(t1), :]], axis=0).astype(BF)
            kr = pl.ds(pl.multiple_of(top - (i + 1) * blk, blk), blk)
            ss.append(lax.dot_general(q, kb[kr, :], nt, preferred_element_type=F32) * scale)
            idx.append((t0, t1, kr))
        for j in range(UP):
            t0, t1, kr = idx[j]
            s0 = jnp.where(pos2 < lens[t0], ss[j][:hq], -jnp.inf)
            s1 = jnp.where(jnp.logical_and(pos2 >= sh, pos2 < sh + lens[t1]), ss[j][hq:], -jnp.inf)
            o = jnp.dot(normal(jnp.concatenate([s0, s1], axis=0)), vb[kr, :], preferred_element_type=F32)
            o2[qrows(t0), :] = o[:hq]
            o2[qrows(t1), :] = o[hq:]
        return c
    kv_wait(0, ns2 * sh)
    lax.fori_loop(0, (ns2 // 2 + UP - 1) // UP, pairs, 0)

    pos = lax.broadcasted_iota(jnp.int32, (hq, l), 1)

    def single(it, c):
        ss, idx = [], []
        for j in range(UL):
            i = jnp.minimum(it * UL + j, nl - 1)
            t = longs[i]
            kr = pl.ds(pl.multiple_of(i * l, l), l)
            ss.append(lax.dot_general(q2[qrows(t), :].astype(BF), kb[kr, :], nt, preferred_element_type=F32) * scale)
            idx.append((t, kr))
        for j in range(UL):
            t, kr = idx[j]
            p = normal(jnp.where(pos < lens[t], ss[j], -jnp.inf))
            o2[qrows(t), :] = jnp.dot(p, vb[kr, :], preferred_element_type=F32)
        return c
    kv_wait(1, nl * l)
    lax.fori_loop(0, (nl + UL - 1) // UL, single, 0)

    for hh in range(hq):
        xa[:, hh * dh:(hh + 1) * dh] = o2[pl.ds(hh, b, stride=hq), :].astype(BF)
    def out(src, dst, j, q):
        cs = pl.ds(j * cq, cq)
        return pltpu.make_async_copy(src.at[:, cs], dst.at[:, cs], out_sem.at[q, j])

    ssq = jnp.zeros((b, 1), F32)
    for j in range(4):
        cs = slice(j * cq, (j + 1) * cq)
        wcopy(wo, j, 1).wait()
        hv = (xv[:, cs].astype(F32) + jnp.dot(xa[...], wb[:, cs], preferred_element_type=F32)).astype(BF)
        h_ref[:, cs] = hv
        out(h_ref, h_hbm, j, 0).start()
        hf = hv.astype(F32)
        ssq += jnp.sum(hf * hf, axis=-1, keepdims=True)
    r = lax.rsqrt(ssq * (1.0 / d) + EPS)
    for j in range(4):
        cs = slice(j * cq, (j + 1) * cq)
        u_ref[:, cs] = (h_ref[:, cs].astype(F32) * r * ln2[cs].astype(F32).reshape(1, cq)).astype(BF)
        out(u_ref, u_hbm, j, 1).start()
    for j in range(4):
        out(h_ref, h_hbm, j, 0).wait()
        out(u_ref, u_hbm, j, 1).wait()


def _attn(x, kk, vv, lens, ln1, ln2, topk, gates, wq, wo):
    b, d = x.shape
    l, dh = kk.shape[1], kk.shape[3]
    hq = wq.shape[1] // dh
    kk, vv = kk.reshape(b, l, dh), vv.reshape(b, l, dh)
    dma = pltpu.SemaphoreType.DMA
    anys = pl.BlockSpec(memory_space=pl.ANY)
    vm = pl.BlockSpec(memory_space=pltpu.VMEM)
    return pl.pallas_call(
        functools.partial(_attn_kernel, (b, l, dh, hq, d)),
        out_shape=(jax.ShapeDtypeStruct((b, d), BF), jax.ShapeDtypeStruct((b, d), BF),
                   jax.ShapeDtypeStruct((16, b), F32)),
        in_specs=[pl.BlockSpec(memory_space=pltpu.SMEM), anys, vm, vm, vm, vm, anys, anys, anys, anys],
        out_specs=(anys, anys, vm),
        scratch_shapes=[
            pltpu.VMEM((b, d), BF), pltpu.VMEM((b, d), BF), dma((2, 4)),
            pltpu.VMEM((b * l, dh), BF), pltpu.VMEM((b * l, dh), BF), pltpu.VMEM((d, d), BF),
            pltpu.VMEM((b * hq, dh), F32), pltpu.VMEM((b * hq, dh), F32),
            pltpu.VMEM((b, d), BF), pltpu.VMEM((b, d), BF),
            pltpu.SMEM((b + 2,), jnp.int32), pltpu.SMEM((b + 2,), jnp.int32),
            dma, dma((2, 2)), dma((2, 4)),
        ],
        compiler_params=pltpu.CompilerParams(vmem_limit_bytes=67043328),
        name='attn',
    )(lens, x, ln1, ln2, topk.T, gates.T, kk, vv, wq, wo)


def _moe_kernel(dims, u_ref, h_ref, rt_ref, ws1, ws3, ws2, w1, w3, w2, y_ref,
                ug, rt, acc, z, xin, s1h, pg, ring_a, ring_b, fb, acc_s, z_s, base, hv, sib, r_d, r_a, r_b,
                keys, gts, loc_sem, a_sem, b_sem, ag_s, ag_r, fw_s, fw_r, rt_s, rt_r, sb_s, sb_r,
                rd_s, rd_r, ra_s, ra_r, rb_s, rb_r):
    b, d, f, edev, cap, ny, nx, kc, chunks, nn = dims
    nk = len(chunks)
    rows = 8 * cap
    half = 2 * cap
    y = lax.axis_index('ey')
    ex = lax.axis_index('ex')
    x = ex // 2
    c = ex % 2
    me = y * nx + ex
    peers = [(y, 2 * (1 - x) + c), (1 - y, 2 * x + c), (1 - y, 2 * (1 - x) + c), (y, 2 * x + 1 - c)]
    pa = ((1 - c) * y + c * (1 - y), 2 * ((1 - c) * (1 - x) + c * x) + c)
    pb = ((1 - c) * (1 - y) + c * y, 2 * ((1 - c) * x + c * (1 - x)) + c)
    chip = y * 2 + x
    chip_a = pa[0] * 2 + pa[1] // 2
    chip_b = pb[0] * 2 + pb[1] // 2
    chip_d = (1 - y) * 2 + 1 - x
    sibling = peers[3]

    def remote(src, dst, ss, rs, dev):
        return pltpu.make_async_remote_copy(src_ref=src, dst_ref=dst, send_sem=ss, recv_sem=rs,
                                            device_id=dev, device_id_type=MESH)

    def urows(k, dev):
        return ug.at[pl.ds(pl.multiple_of(dev * b, b), b), pl.ds(*chunks[k])]

    def ag(k, j):
        return remote(u_ref.at[:, pl.ds(*chunks[k])], urows(k, me), ag_s.at[k, j], ag_r.at[k, j], peers[j])

    def fw(k, j):
        src = peers[j][0] * nx + peers[j][1]
        return remote(urows(k, src), urows(k, src), fw_s.at[k, j], fw_r.at[k, j], sibling)

    def rts(i):
        t = lax.rem(me + i, 8)
        return remote(rt_ref, rt.at[me], rt_s.at[i - 1], rt_r.at[i - 1], (t // nx, lax.rem(t, nx)))

    def copy_a(slot, start, size, e):
        ks = pl.ds(start, size)
        s1 = ws1.at[ks] if e is None else w1.at[e, ks]
        s3 = ws3.at[ks] if e is None else w3.at[e, ks]
        return (pltpu.make_async_copy(s1, ring_a.at[slot, pl.ds(0, size), pl.ds(0, f)], a_sem.at[slot, 0]),
                pltpu.make_async_copy(s3, ring_a.at[slot, pl.ds(0, size), pl.ds(f, f)], a_sem.at[slot, 1]))

    def shared_a(i):
        start = i * kc if isinstance(i, int) else pl.multiple_of(i * kc, kc)
        return copy_a(i, start, kc, None)

    def copy_b(t, n, e):
        slot = t % NB if isinstance(t, int) else lax.rem(t, NB)
        ns = pl.ds(n * NC if isinstance(n, int) else pl.multiple_of(n * NC, NC), NC)
        src = ws2.at[:, ns] if e is None else w2.at[e, :, ns]
        return pltpu.make_async_copy(src, ring_b.at[slot], b_sem.at[slot])

    for t in range(NA):
        for q in copy_a(t, *chunks[0], t):
            q.start()
    own = pltpu.make_async_copy(u_ref, ug.at[pl.ds(pl.multiple_of(me * b, b), b)], loc_sem.at[0])
    own.start()
    own_h = pltpu.make_async_copy(h_ref, hv, loc_sem.at[1])
    own_h.start()
    own_rt = pltpu.make_async_copy(rt_ref, rt.at[me], loc_sem.at[2])
    own_rt.start()
    for t in range(NB):
        copy_b(t, 0, t).start()

    barrier = pltpu.get_barrier_semaphore()
    for i in range(1, 8):
        t = lax.rem(me + i, 8)
        pl.semaphore_signal(barrier, inc=1, device_id=(t // nx, lax.rem(t, nx)), device_id_type=MESH)
    pl.semaphore_wait(barrier, 7)

    for i in range(1, 8):
        rts(i).start()
    for k in range(nk):
        for j in (2, 0, 1, 3):
            ag(k, j).start()

    def swiglu(g, v):
        return (g * (1.0 / (1.0 + jnp.exp(-g))) * v).astype(BF)

    own_rt.wait()
    for i in range(1, 8):
        rts(i).wait_recv()
    for s in range(8):
        tk = rt[s, 0:8, :]
        gt = rt[s, 8:16, :]
        for e in range(edev):
            m = tk == (me * edev + e).astype(F32)
            keys[s * edev + e:s * edev + e + 1, :] = jnp.sum(jnp.where(m, 1.0, 0.0), axis=0, keepdims=True)
            gts[s * edev + e:s * edev + e + 1, :] = jnp.sum(jnp.where(m, gt, 0.0), axis=0, keepdims=True)
    chosen = keys[...]
    before = (lax.broadcasted_iota(jnp.int32, (b, b), 0) < lax.broadcasted_iota(jnp.int32, (b, b), 1))
    rank = jnp.dot(chosen.astype(BF), jnp.where(before, 1.0, 0.0).astype(BF), preferred_element_type=F32)
    keys[...] = jnp.where(chosen > 0.0, rank, -1.0)
    slot_no = lax.broadcasted_iota(jnp.int32, (cap, b), 0).astype(F32)
    zero = jnp.zeros((cap, b), F32)
    for p in range(4):
        parts = []
        for e in range(edev):
            i0, i1 = 2 * p * edev + e, (2 * p + 1) * edev + e
            one0 = jnp.where(keys[i0:i0 + 1, :] == slot_no, 1.0, 0.0)
            one1 = jnp.where(keys[i1:i1 + 1, :] == slot_no, 1.0, 0.0)
            s1h[p, e * half:(e + 1) * half, :] = jnp.concatenate(
                [jnp.concatenate([one0, zero], axis=1), jnp.concatenate([zero, one1], axis=1)], axis=0).astype(BF)
            parts.append(jnp.concatenate(
                [jnp.concatenate([one0 * gts[i0:i0 + 1, :], zero], axis=1),
                 jnp.concatenate([zero, one1 * gts[i1:i1 + 1, :]], axis=1)], axis=0))
        g = jnp.concatenate(parts, axis=0).T
        hi = g.astype(BF)
        rest = g - hi.astype(F32)
        mid = rest.astype(BF)
        lo = (rest - mid.astype(F32)).astype(BF)
        pg[p, 0:2 * b, :] = hi
        pg[p, 2 * b:4 * b, :] = mid
        pg[p, 4 * b:6 * b, :] = lo

    def forward(k):
        for j in range(3):
            ag(k, j).wait_recv()
            fw(k, j).start()

    forward(0)
    own.wait()
    for k in range(nk):
        ag(k, 3).wait_recv()
        for j in range(3):
            fw(k, j).wait_recv()
        start, size = chunks[k]
        for p in range(4):
            dsp = jnp.dot(s1h[p], ug[p * 2 * b:(p + 1) * 2 * b, start:start + size],
                          preferred_element_type=F32).astype(BF)
            for e in range(edev):
                xin[e, p * half:(p + 1) * half, 0:size] = dsp[e * half:(e + 1) * half]

        def expert(e, carry, k=k, start=start, size=size, late=False):
            slot = lax.rem(e, NA)
            for q in copy_a(slot, start, size, e):
                q.wait()
            rs = pl.ds(pl.multiple_of(e * rows, rows), rows)
            r = jnp.dot(xin[e, :, 0:size], ring_a[slot, 0:size, :], preferred_element_type=F32)
            if k == 0:
                acc[rs, :] = r
            else:
                acc[rs, :] += r
            if not late:
                nxt = copy_a(slot, start, size, e + NA)
            elif k + 1 < nk:
                nxt = copy_a(slot, *chunks[k + 1], e + NA - edev)
            else:
                nxt = shared_a(slot)
            for q in nxt:
                q.start()
            if k == nk - 1:
                z[e] = swiglu(acc[rs, pl.ds(0, f)], acc[rs, pl.ds(f, f)])
            return carry
        lax.fori_loop(0, edev - NA, expert, 0)
        if k + 1 < nk:
            forward(k + 1)
        lax.fori_loop(edev - NA, edev, functools.partial(expert, late=True), 0)

    def part(n, core, p):
        col = (core * 4 + p) * NC
        col = col if isinstance(col, int) else pl.multiple_of(col, NC)
        return (pl.ds(pl.multiple_of(n * b, b), b), pl.ds(col, NC))

    def to_sib(n):
        src = acc.at[pl.ds(pl.multiple_of(n * b, b), b), pl.ds(pl.multiple_of((1 - c) * 4 * NC, 4 * NC), 4 * NC)]
        return remote(src, sib.at[n], sb_s.at[n], sb_r.at[n], sibling)

    def send_d(n):
        return remote(acc.at[part(n, c, chip_d)], r_d.at[n], rd_s.at[n], rd_r.at[n], pa)

    def send_a(n):
        return remote(acc.at[part(n, c, chip_a)], r_a.at[n], ra_s.at[n], ra_r.at[n], pa)

    def send_b(n):
        return remote(acc.at[part(n, c, chip_b)], r_b.at[n], rb_s.at[n], rb_r.at[n], pb)

    def both(n, p):
        return acc[part(n, c, p)] + sib[n, :, pl.ds(pl.multiple_of(p * NC, NC), NC)]

    def stage1(n):
        to_sib(n).wait_recv()
        acc[part(n, c, chip_d)] = both(n, chip_d)
        send_d(n).start()
        acc[part(n, c, chip_a)] = both(n, chip_a)
        send_a(n).start()
        base[n] = both(n, chip)

    def stage2(n):
        send_d(n).wait_recv()
        acc[part(n, c, chip_b)] = both(n, chip_b) + r_d[n]
        send_b(n).start()

    def block(n, carry):
        def down(e2, cc):
            es = [e2 * ND + j for j in range(ND)]
            for e in es:
                copy_b(n * edev + e, n, e).wait()
            rs = [jnp.dot(z[e], ring_b[lax.rem(n * edev + e, NB)], preferred_element_type=F32).astype(BF) for e in es]
            for e, r in zip(es, rs):
                for p in range(4):
                    fb[p, pl.ds(pl.multiple_of(e * half, half), half), :] = r[p * half:(p + 1) * half]
            for e in es:
                i2 = n * edev + e + NB

                @pl.when(i2 < nn * edev)
                def _():
                    copy_b(i2, i2 // edev, lax.rem(i2, edev)).start()

                @pl.when(i2 >= nn * edev)
                def _():
                    copy_b(i2, i2 - nn * edev, None).start()
            return cc
        lax.fori_loop(0, edev // 2 // ND, down, 0)

        @pl.when(n > 0)
        def _():
            stage1(n - 1)
        lax.fori_loop(edev // 2 // ND, edev // ND, down, 0)
        for p in range(4):
            q = jnp.dot(pg[p], fb[p], preferred_element_type=F32)
            q = q[0:2 * b] + q[2 * b:4 * b] + q[4 * b:6 * b]
            for core in range(2):
                acc[part(n, core, p)] = q[core * b:(core + 1) * b]
        to_sib(n).start()

        @pl.when(n > 1)
        def _():
            stage2(n - 2)
        return carry
    lax.fori_loop(0, nn, block, 0)
    stage1(nn - 1)
    stage2(nn - 2)

    for i in range(d // kc):
        for q in shared_a(i):
            q.wait()
        r = jnp.dot(ug[pl.ds(pl.multiple_of(me * b, b), b), i * kc:(i + 1) * kc], ring_a[i],
                    preferred_element_type=F32)
        if i == 0:
            acc_s[...] = r
        else:
            acc_s[...] += r
    z_s[...] = swiglu(acc_s[:, :f], acc_s[:, f:])
    stage2(nn - 1)
    own_h.wait()
    for n in range(nn):
        t = nn * edev + n
        copy_b(t, n, None).wait()
        sh = jnp.dot(z_s[...], ring_b[t % NB], preferred_element_type=F32).astype(BF).astype(F32)
        base[n] += hv[:, n * NC:(n + 1) * NC].astype(F32) + sh
        if n + NB < nn:
            copy_b(t + NB, n + NB, None).start()

    def out(n):
        cs = pl.ds(n * NC, NC)
        return pltpu.make_async_copy(hv.at[:, cs], y_ref.at[:, cs], b_sem.at[n])

    for n in range(nn):
        send_a(n).wait_recv()
        send_b(n).wait_recv()
        hv[:, n * NC:(n + 1) * NC] = (base[n] + r_a[n] + r_b[n]).astype(BF)
        out(n).start()
    for n in range(nn):
        out(n).wait()
    for i in range(1, 8):
        rts(i).wait_send()
    for k in range(nk):
        for j in range(4):
            ag(k, j).wait_send()
        for j in range(3):
            fw(k, j).wait_send()
    for n in range(nn):
        to_sib(n).wait_send()
        send_d(n).wait_send()
        send_a(n).wait_send()
        send_b(n).wait_send()


def _moe(u, h, rt, ws1, ws3, ws2, w1, w3, w2, ny, nx):
    b, d = u.shape
    edev, _, f = w1.shape
    cap = 24
    kc, nn = 512, d // NC
    chunks = ((0, 256), (256, 256), (512, 512), (1024, 512), (1536, 512))
    nk = len(chunks)
    dims = (b, d, f, edev, cap, ny, nx, kc, chunks, nn)
    dma = pltpu.SemaphoreType.DMA
    anys = pl.BlockSpec(memory_space=pl.ANY)
    return pl.pallas_call(
        functools.partial(_moe_kernel, dims),
        out_shape=jax.ShapeDtypeStruct((b, d), BF),
        in_specs=[anys] * 9,
        out_specs=anys,
        scratch_shapes=[
            pltpu.VMEM((8 * b, d), BF),
            pltpu.VMEM((8, 16, b), F32),
            pltpu.VMEM((edev * 8 * cap, 2 * f), F32),
            pltpu.VMEM((edev, 8 * cap, f), BF),
            pltpu.VMEM((edev, 8 * cap, kc), BF),
            pltpu.VMEM((4, edev * 2 * cap, 2 * b), BF),
            pltpu.VMEM((4, 6 * b, edev * 2 * cap), BF),
            pltpu.VMEM((NA, kc, 2 * f), BF),
            pltpu.VMEM((NB, f, NC), BF),
            pltpu.VMEM((4, edev * 2 * cap, NC), BF),
            pltpu.VMEM((b, 2 * f), F32),
            pltpu.VMEM((b, f), BF),
            pltpu.VMEM((nn, b, NC), F32),
            pltpu.VMEM((b, d), BF),
            pltpu.VMEM((nn, b, 4 * NC), F32),
            pltpu.VMEM((nn, b, NC), F32),
            pltpu.VMEM((nn, b, NC), F32),
            pltpu.VMEM((nn, b, NC), F32),
            pltpu.VMEM((8 * edev, b), F32),
            pltpu.VMEM((8 * edev, b), F32),
            dma((3,)), dma((NA, 2)), dma((NB,)),
            dma((nk, 4)), dma((nk, 4)), dma((nk, 3)), dma((nk, 3)), dma((7,)), dma((7,)),
            dma((nn,)), dma((nn,)), dma((nn,)), dma((nn,)), dma((nn,)), dma((nn,)), dma((nn,)), dma((nn,)),
        ],
        compiler_params=pltpu.CompilerParams(collective_id=0, has_side_effects=True, vmem_limit_bytes=67043328),
        name='moe',
    )(u, h, rt, ws1, ws3, ws2, w1, w3, w2)


def solution(mesh):
    ey, ex = mesh.shape['ey'], mesh.shape['ex']
    rows = P(('ey', 'ex'))
    rep = P()

    def local(x, kv_k, kv_v, lens, topk_idx, gates, ln1, ln2, wq, wo, ws1, ws3, ws2, w1, w3, w2):
        h, u, rt = _attn(x, kv_k, kv_v, lens, ln1, ln2, topk_idx, gates, wq, wo)
        return _moe(u, h, rt, ws1, ws3, ws2, w1, w3, w2, ey, ex)

    return jax.shard_map(
        local, mesh=mesh,
        in_specs=(rows, rows, rows, rows, rows, rows, rep, rep, rep, rep, rep, rep, rep, rows, rows, rows),
        out_specs=rows, check_vma=False)
```

```python
import functools

import jax
import jax.numpy as jnp
from jax import lax
from jax.experimental import pallas as pl
from jax.experimental.pallas import tpu as pltpu
from jax.sharding import PartitionSpec as P

EPS = 1e-6
BF = jnp.bfloat16
F32 = jnp.float32
MESH = pl.DeviceIdType.MESH

NA = 4
NB = 8
ND = 4
NC = 256
UP = 24
UL = 24


def _attn_kernel(dims, lens, x_hbm, ln1, ln2, topk, gates, kk, vv, wq, wo, h_hbm, u_hbm, rt_ref,
                 h_ref, u_ref, out_sem, kb, vb, wb, q2, o2, xa, xv, shorts, longs, x_sem, kv_sem, w_sem):
    b, l, dh, hq, d = dims
    sh = 64
    blk = 2 * sh
    cq = d // 4
    top = b * l

    xcopy = pltpu.make_async_copy(x_hbm, xv, x_sem)
    xcopy.start()

    def wcopy(w, i, s):
        return pltpu.make_async_copy(w.at[:, pl.ds(i * cq, cq)], wb.at[:, pl.ds(i * cq, cq)], w_sem.at[s, i])

    for i in range(4):
        wcopy(wq, i, 0).start()

    def srow(i):
        return pl.multiple_of(top - (i // 2 + 1) * blk + lax.rem(i, 2) * sh, sh)

    def kv_s(t, i):
        for q, (src, dst) in enumerate(((kk, kb), (vv, vb))):
            pltpu.make_async_copy(src.at[t, pl.ds(0, sh)], dst.at[pl.ds(srow(i), sh)], kv_sem.at[0, q]).start()

    def kv_l(t, i):
        for q, (src, dst) in enumerate(((kk, kb), (vv, vb))):
            pltpu.make_async_copy(src.at[t], dst.at[pl.ds(pl.multiple_of(i * l, l), l)], kv_sem.at[1, q]).start()

    def kv_wait(kind, n_rows):
        r = pl.ds(0, pl.multiple_of(n_rows, sh))
        for q, buf in enumerate((kb, vb)):
            pltpu.make_async_copy(buf.at[r], buf.at[r], kv_sem.at[kind, q]).wait()

    def sort_rows(t, c):
        cs, cl = c
        short = lens[t] <= sh
        shorts[cs] = t
        longs[cl] = t
        one = (lens[t] <= sh).astype(jnp.int32)
        return cs + one, cl + 1 - one
    ns, nl = lax.fori_loop(0, b, sort_rows, (0, 0), unroll=4)
    last = shorts[jnp.maximum(ns - 1, 0)]
    shorts[ns] = last
    ns2 = ns + lax.rem(ns, 2)

    def issue_s(i, carry):
        kv_s(shorts[i], i)
        return carry
    lax.fori_loop(0, ns2, issue_s, 0)

    def issue_l(i, carry):
        kv_l(longs[i], i)
        return carry
    lax.fori_loop(0, nl, issue_l, 0)

    k = topk.shape[0]
    rt_ref[...] = jnp.concatenate(
        [topk[...].astype(F32), jnp.full((8 - k, b), -1.0, F32), gates[...], jnp.zeros((8 - k, b), F32)], axis=0)
    xcopy.wait()
    x = xv[...].astype(F32)
    r = lax.rsqrt(jnp.mean(x * x, axis=-1, keepdims=True) + EPS)
    xa[...] = (x * r * ln1[...].astype(F32).reshape(1, d)).astype(BF)
    for j in range(4):
        wcopy(wq, j, 0).wait()
        q = jnp.dot(xa[...], wb[:, j * cq:(j + 1) * cq], preferred_element_type=F32)
        for hh in range(cq // dh):
            q2[pl.ds(j * (cq // dh) + hh, b, stride=hq), :] = q[:, hh * dh:(hh + 1) * dh].astype(BF).astype(F32)
        wcopy(wo, j, 1).start()

    def qrows(t):
        return pl.ds(pl.multiple_of(t * hq, hq), hq)

    def normal(s):
        e = jnp.exp(s - jnp.max(s, axis=-1, keepdims=True))
        return (e * (1.0 / jnp.sum(e, axis=-1, keepdims=True))).astype(BF)

    nt = (((1,), (1,)), ((), ()))
    pos2 = lax.broadcasted_iota(jnp.int32, (hq, blk), 1)
    scale = dh ** -0.5

    def pairs(it, c):
        ss, idx = [], []
        for j in range(UP):
            i = jnp.minimum(it * UP + j, (ns2 // 2) - 1)
            t0, t1 = shorts[2 * i], shorts[2 * i + 1]
            q = jnp.concatenate([q2[qrows(t0), :], q2[qrows(t1), :]], axis=0).astype(BF)
            kr = pl.ds(pl.multiple_of(top - (i + 1) * blk, blk), blk)
            ss.append(lax.dot_general(q, kb[kr, :], nt, preferred_element_type=F32) * scale)
            idx.append((t0, t1, kr))
        for j in range(UP):
            t0, t1, kr = idx[j]
            s0 = jnp.where(pos2 < lens[t0], ss[j][:hq], -jnp.inf)
            s1 = jnp.where(jnp.logical_and(pos2 >= sh, pos2 < sh + lens[t1]), ss[j][hq:], -jnp.inf)
            o = jnp.dot(normal(jnp.concatenate([s0, s1], axis=0)), vb[kr, :], preferred_element_type=F32)
            o2[qrows(t0), :] = o[:hq]
            o2[qrows(t1), :] = o[hq:]
        return c
    kv_wait(0, ns2 * sh)
    lax.fori_loop(0, (ns2 // 2 + UP - 1) // UP, pairs, 0)

    pos = lax.broadcasted_iota(jnp.int32, (hq, l), 1)

    def single(it, c):
        ss, idx = [], []
        for j in range(UL):
            i = jnp.minimum(it * UL + j, nl - 1)
            t = longs[i]
            kr = pl.ds(pl.multiple_of(i * l, l), l)
            ss.append(lax.dot_general(q2[qrows(t), :].astype(BF), kb[kr, :], nt, preferred_element_type=F32) * scale)
            idx.append((t, kr))
        for j in range(UL):
            t, kr = idx[j]
            p = normal(jnp.where(pos < lens[t], ss[j], -jnp.inf))
            o2[qrows(t), :] = jnp.dot(p, vb[kr, :], preferred_element_type=F32)
        return c
    kv_wait(1, nl * l)
    lax.fori_loop(0, (nl + UL - 1) // UL, single, 0)

    for hh in range(hq):
        xa[:, hh * dh:(hh + 1) * dh] = o2[pl.ds(hh, b, stride=hq), :].astype(BF)
    def out(src, dst, j, q):
        cs = pl.ds(j * cq, cq)
        return pltpu.make_async_copy(src.at[:, cs], dst.at[:, cs], out_sem.at[q, j])

    ssq = jnp.zeros((b, 1), F32)
    for j in range(4):
        cs = slice(j * cq, (j + 1) * cq)
        wcopy(wo, j, 1).wait()
        hv = (xv[:, cs].astype(F32) + jnp.dot(xa[...], wb[:, cs], preferred_element_type=F32)).astype(BF)
        h_ref[:, cs] = hv
        out(h_ref, h_hbm, j, 0).start()
        hf = hv.astype(F32)
        ssq += jnp.sum(hf * hf, axis=-1, keepdims=True)
    r = lax.rsqrt(ssq * (1.0 / d) + EPS)
    for j in range(4):
        cs = slice(j * cq, (j + 1) * cq)
        u_ref[:, cs] = (h_ref[:, cs].astype(F32) * r * ln2[cs].astype(F32).reshape(1, cq)).astype(BF)
        out(u_ref, u_hbm, j, 1).start()
    for j in range(4):
        out(h_ref, h_hbm, j, 0).wait()
        out(u_ref, u_hbm, j, 1).wait()


def _attn(x, kk, vv, lens, ln1, ln2, topk, gates, wq, wo):
    b, d = x.shape
    l, dh = kk.shape[1], kk.shape[3]
    hq = wq.shape[1] // dh
    kk, vv = kk.reshape(b, l, dh), vv.reshape(b, l, dh)
    dma = pltpu.SemaphoreType.DMA
    anys = pl.BlockSpec(memory_space=pl.ANY)
    vm = pl.BlockSpec(memory_space=pltpu.VMEM)
    return pl.pallas_call(
        functools.partial(_attn_kernel, (b, l, dh, hq, d)),
        out_shape=(jax.ShapeDtypeStruct((b, d), BF), jax.ShapeDtypeStruct((b, d), BF),
                   jax.ShapeDtypeStruct((16, b), F32)),
        in_specs=[pl.BlockSpec(memory_space=pltpu.SMEM), anys, vm, vm, vm, vm, anys, anys, anys, anys],
        out_specs=(anys, anys, vm),
        scratch_shapes=[
            pltpu.VMEM((b, d), BF), pltpu.VMEM((b, d), BF), dma((2, 4)),
            pltpu.VMEM((b * l, dh), BF), pltpu.VMEM((b * l, dh), BF), pltpu.VMEM((d, d), BF),
            pltpu.VMEM((b * hq, dh), F32), pltpu.VMEM((b * hq, dh), F32),
            pltpu.VMEM((b, d), BF), pltpu.VMEM((b, d), BF),
            pltpu.SMEM((b + 2,), jnp.int32), pltpu.SMEM((b + 2,), jnp.int32),
            dma, dma((2, 2)), dma((2, 4)),
        ],
        compiler_params=pltpu.CompilerParams(vmem_limit_bytes=67043328),
        name='attn',
    )(lens, x, ln1, ln2, topk.T, gates.T, kk, vv, wq, wo)


def _moe_kernel(dims, u_ref, h_ref, rt_ref, ws1, ws3, ws2, w1, w3, w2, y_ref,
                ug, rt, acc, z, xin, s1h, pg, ring_a, ring_b, fb, acc_s, z_s, base, hv, sib, r_d, r_a, r_b,
                keys, gts, loc_sem, a_sem, b_sem, ag_s, ag_r, fw_s, fw_r, rt_s, rt_r, sb_s, sb_r,
                rd_s, rd_r, ra_s, ra_r, rb_s, rb_r):
    b, d, f, edev, cap, ny, nx, kc, chunks, nn = dims
    nk = len(chunks)
    rows = 8 * cap
    half = 2 * cap
    y = lax.axis_index('ey')
    ex = lax.axis_index('ex')
    x = ex // 2
    c = ex % 2
    me = y * nx + ex
    peers = [(y, 2 * (1 - x) + c), (1 - y, 2 * x + c), (1 - y, 2 * (1 - x) + c), (y, 2 * x + 1 - c)]
    pa = ((1 - c) * y + c * (1 - y), 2 * ((1 - c) * (1 - x) + c * x) + c)
    pb = ((1 - c) * (1 - y) + c * y, 2 * ((1 - c) * x + c * (1 - x)) + c)
    chip = y * 2 + x
    chip_a = pa[0] * 2 + pa[1] // 2
    chip_b = pb[0] * 2 + pb[1] // 2
    chip_d = (1 - y) * 2 + 1 - x
    sibling = peers[3]

    def remote(src, dst, ss, rs, dev):
        return pltpu.make_async_remote_copy(src_ref=src, dst_ref=dst, send_sem=ss, recv_sem=rs,
                                            device_id=dev, device_id_type=MESH)

    def urows(k, dev):
        return ug.at[pl.ds(pl.multiple_of(dev * b, b), b), pl.ds(*chunks[k])]

    def ag(k, j):
        return remote(u_ref.at[:, pl.ds(*chunks[k])], urows(k, me), ag_s.at[k, j], ag_r.at[k, j], peers[j])

    def fw(k, j):
        src = peers[j][0] * nx + peers[j][1]
        return remote(urows(k, src), urows(k, src), fw_s.at[k, j], fw_r.at[k, j], sibling)

    def rts(i):
        t = lax.rem(me + i, 8)
        return remote(rt_ref, rt.at[me], rt_s.at[i - 1], rt_r.at[i - 1], (t // nx, lax.rem(t, nx)))

    def copy_a(slot, start, size, e):
        ks = pl.ds(start, size)
        s1 = ws1.at[ks] if e is None else w1.at[e, ks]
        s3 = ws3.at[ks] if e is None else w3.at[e, ks]
        return (pltpu.make_async_copy(s1, ring_a.at[slot, pl.ds(0, size), pl.ds(0, f)], a_sem.at[slot, 0]),
                pltpu.make_async_copy(s3, ring_a.at[slot, pl.ds(0, size), pl.ds(f, f)], a_sem.at[slot, 1]))

    def shared_a(i):
        start = i * kc if isinstance(i, int) else pl.multiple_of(i * kc, kc)
        return copy_a(i, start, kc, None)

    def copy_b(t, n, e):
        slot = t % NB if isinstance(t, int) else lax.rem(t, NB)
        ns = pl.ds(n * NC if isinstance(n, int) else pl.multiple_of(n * NC, NC), NC)
        src = ws2.at[:, ns] if e is None else w2.at[e, :, ns]
        return pltpu.make_async_copy(src, ring_b.at[slot], b_sem.at[slot])

    for t in range(NA):
        for q in copy_a(t, *chunks[0], t):
            q.start()
    own = pltpu.make_async_copy(u_ref, ug.at[pl.ds(pl.multiple_of(me * b, b), b)], loc_sem.at[0])
    own.start()
    own_h = pltpu.make_async_copy(h_ref, hv, loc_sem.at[1])
    own_h.start()
    own_rt = pltpu.make_async_copy(rt_ref, rt.at[me], loc_sem.at[2])
    own_rt.start()
    for t in range(NB):
        copy_b(t, 0, t).start()

    barrier = pltpu.get_barrier_semaphore()
    for i in range(1, 8):
        t = lax.rem(me + i, 8)
        pl.semaphore_signal(barrier, inc=1, device_id=(t // nx, lax.rem(t, nx)), device_id_type=MESH)
    pl.semaphore_wait(barrier, 7)

    for i in range(1, 8):
        rts(i).start()
    for k in range(nk):
        for j in (2, 0, 1, 3):
            ag(k, j).start()

    def swiglu(g, v):
        return (g * (1.0 / (1.0 + jnp.exp(-g))) * v).astype(BF)

    own_rt.wait()
    for i in range(1, 8):
        rts(i).wait_recv()
    for s in range(8):
        tk = rt[s, 0:8, :]
        gt = rt[s, 8:16, :]
        for e in range(edev):
            m = tk == (me * edev + e).astype(F32)
            keys[s * edev + e:s * edev + e + 1, :] = jnp.sum(jnp.where(m, 1.0, 0.0), axis=0, keepdims=True)
            gts[s * edev + e:s * edev + e + 1, :] = jnp.sum(jnp.where(m, gt, 0.0), axis=0, keepdims=True)
    chosen = keys[...]
    before = (lax.broadcasted_iota(jnp.int32, (b, b), 0) < lax.broadcasted_iota(jnp.int32, (b, b), 1))
    rank = jnp.dot(chosen.astype(BF), jnp.where(before, 1.0, 0.0).astype(BF), preferred_element_type=F32)
    keys[...] = jnp.where(chosen > 0.0, rank, -1.0)
    slot_no = lax.broadcasted_iota(jnp.int32, (cap, b), 0).astype(F32)
    zero = jnp.zeros((cap, b), F32)
    for p in range(4):
        parts = []
        for e in range(edev):
            i0, i1 = 2 * p * edev + e, (2 * p + 1) * edev + e
            one0 = jnp.where(keys[i0:i0 + 1, :] == slot_no, 1.0, 0.0)
            one1 = jnp.where(keys[i1:i1 + 1, :] == slot_no, 1.0, 0.0)
            s1h[p, e * half:(e + 1) * half, :] = jnp.concatenate(
                [jnp.concatenate([one0, zero], axis=1), jnp.concatenate([zero, one1], axis=1)], axis=0).astype(BF)
            parts.append(jnp.concatenate(
                [jnp.concatenate([one0 * gts[i0:i0 + 1, :], zero], axis=1),
                 jnp.concatenate([zero, one1 * gts[i1:i1 + 1, :]], axis=1)], axis=0))
        g = jnp.concatenate(parts, axis=0).T
        hi = g.astype(BF)
        rest = g - hi.astype(F32)
        mid = rest.astype(BF)
        lo = (rest - mid.astype(F32)).astype(BF)
        pg[p, 0:2 * b, :] = hi
        pg[p, 2 * b:4 * b, :] = mid
        pg[p, 4 * b:6 * b, :] = lo

    def forward(k):
        for j in (2, 0, 1):
            ag(k, j).wait_recv()
            fw(k, j).start()

    forward(0)
    own.wait()
    for k in range(nk):
        ag(k, 3).wait_recv()
        for j in range(3):
            fw(k, j).wait_recv()
        start, size = chunks[k]
        for p in range(4):
            dsp = jnp.dot(s1h[p], ug[p * 2 * b:(p + 1) * 2 * b, start:start + size],
                          preferred_element_type=F32).astype(BF)
            for e in range(edev):
                xin[e, p * half:(p + 1) * half, 0:size] = dsp[e * half:(e + 1) * half]

        def expert(e, carry, k=k, start=start, size=size, late=False):
            slot = lax.rem(e, NA)
            for q in copy_a(slot, start, size, e):
                q.wait()
            rs = pl.ds(pl.multiple_of(e * rows, rows), rows)
            r = jnp.dot(xin[e, :, 0:size], ring_a[slot, 0:size, :], preferred_element_type=F32)
            if k == 0:
                acc[rs, :] = r
            else:
                acc[rs, :] += r
            if not late:
                nxt = copy_a(slot, start, size, e + NA)
            elif k + 1 < nk:
                nxt = copy_a(slot, *chunks[k + 1], e + NA - edev)
            else:
                nxt = shared_a(slot)
            for q in nxt:
                q.start()
            if k == nk - 1:
                z[e] = swiglu(acc[rs, pl.ds(0, f)], acc[rs, pl.ds(f, f)])
            return carry
        lax.fori_loop(0, edev - NA, expert, 0)
        if k + 1 < nk:
            forward(k + 1)
        lax.fori_loop(edev - NA, edev, functools.partial(expert, late=True), 0)

    def part(n, core, p):
        col = (core * 4 + p) * NC
        col = col if isinstance(col, int) else pl.multiple_of(col, NC)
        return (pl.ds(pl.multiple_of(n * b, b), b), pl.ds(col, NC))

    def to_sib(n):
        src = acc.at[pl.ds(pl.multiple_of(n * b, b), b), pl.ds(pl.multiple_of((1 - c) * 4 * NC, 4 * NC), 4 * NC)]
        return remote(src, sib.at[n], sb_s.at[n], sb_r.at[n], sibling)

    def send_d(n):
        return remote(acc.at[part(n, c, chip_d)], r_d.at[n], rd_s.at[n], rd_r.at[n], pa)

    def send_a(n):
        return remote(acc.at[part(n, c, chip_a)], r_a.at[n], ra_s.at[n], ra_r.at[n], pa)

    def send_b(n):
        return remote(acc.at[part(n, c, chip_b)], r_b.at[n], rb_s.at[n], rb_r.at[n], pb)

    def both(n, p):
        return acc[part(n, c, p)] + sib[n, :, pl.ds(pl.multiple_of(p * NC, NC), NC)]

    def stage1(n):
        to_sib(n).wait_recv()
        acc[part(n, c, chip_d)] = both(n, chip_d)
        send_d(n).start()
        acc[part(n, c, chip_a)] = both(n, chip_a)
        send_a(n).start()
        base[n] = both(n, chip)

    def stage2(n):
        send_d(n).wait_recv()
        acc[part(n, c, chip_b)] = both(n, chip_b) + r_d[n]
        send_b(n).start()

    def block(n, carry):
        def down(e2, cc):
            es = [e2 * ND + j for j in range(ND)]
            for e in es:
                copy_b(n * edev + e, n, e).wait()
            rs = [jnp.dot(z[e], ring_b[lax.rem(n * edev + e, NB)], preferred_element_type=F32).astype(BF) for e in es]
            for e, r in zip(es, rs):
                for p in range(4):
                    fb[p, pl.ds(pl.multiple_of(e * half, half), half), :] = r[p * half:(p + 1) * half]
            for e in es:
                i2 = n * edev + e + NB

                @pl.when(i2 < nn * edev)
                def _():
                    copy_b(i2, i2 // edev, lax.rem(i2, edev)).start()

                @pl.when(i2 >= nn * edev)
                def _():
                    copy_b(i2, i2 - nn * edev, None).start()
            return cc
        lax.fori_loop(0, edev // 2 // ND, down, 0)

        @pl.when(n > 0)
        def _():
            stage1(n - 1)
        lax.fori_loop(edev // 2 // ND, edev // ND, down, 0)
        for p in range(4):
            q = jnp.dot(pg[p], fb[p], preferred_element_type=F32)
            q = q[0:2 * b] + q[2 * b:4 * b] + q[4 * b:6 * b]
            for core in range(2):
                acc[part(n, core, p)] = q[core * b:(core + 1) * b]
        to_sib(n).start()

        @pl.when(n > 1)
        def _():
            stage2(n - 2)
        return carry
    lax.fori_loop(0, nn, block, 0)
    stage1(nn - 1)
    stage2(nn - 2)

    for i in range(d // kc):
        for q in shared_a(i):
            q.wait()
        r = jnp.dot(ug[pl.ds(pl.multiple_of(me * b, b), b), i * kc:(i + 1) * kc], ring_a[i],
                    preferred_element_type=F32)
        if i == 0:
            acc_s[...] = r
        else:
            acc_s[...] += r
    z_s[...] = swiglu(acc_s[:, :f], acc_s[:, f:])
    stage2(nn - 1)
    own_h.wait()
    for n in range(nn):
        t = nn * edev + n
        copy_b(t, n, None).wait()
        sh = jnp.dot(z_s[...], ring_b[t % NB], preferred_element_type=F32).astype(BF).astype(F32)
        base[n] += hv[:, n * NC:(n + 1) * NC].astype(F32) + sh
        if n + NB < nn:
            copy_b(t + NB, n + NB, None).start()

    def out(n):
        cs = pl.ds(n * NC, NC)
        return pltpu.make_async_copy(hv.at[:, cs], y_ref.at[:, cs], b_sem.at[n])

    for n in range(nn):
        send_a(n).wait_recv()
        send_b(n).wait_recv()
        hv[:, n * NC:(n + 1) * NC] = (base[n] + r_a[n] + r_b[n]).astype(BF)
        out(n).start()
    for n in range(nn):
        out(n).wait()
    for i in range(1, 8):
        rts(i).wait_send()
    for k in range(nk):
        for j in range(4):
            ag(k, j).wait_send()
        for j in range(3):
            fw(k, j).wait_send()
    for n in range(nn):
        to_sib(n).wait_send()
        send_d(n).wait_send()
        send_a(n).wait_send()
        send_b(n).wait_send()


def _moe(u, h, rt, ws1, ws3, ws2, w1, w3, w2, ny, nx):
    b, d = u.shape
    edev, _, f = w1.shape
    cap = 24
    kc, nn = 512, d // NC
    chunks = ((0, 256), (256, 256), (512, 512), (1024, 512), (1536, 512))
    nk = len(chunks)
    dims = (b, d, f, edev, cap, ny, nx, kc, chunks, nn)
    dma = pltpu.SemaphoreType.DMA
    anys = pl.BlockSpec(memory_space=pl.ANY)
    return pl.pallas_call(
        functools.partial(_moe_kernel, dims),
        out_shape=jax.ShapeDtypeStruct((b, d), BF),
        in_specs=[anys] * 9,
        out_specs=anys,
        scratch_shapes=[
            pltpu.VMEM((8 * b, d), BF),
            pltpu.VMEM((8, 16, b), F32),
            pltpu.VMEM((edev * 8 * cap, 2 * f), F32),
            pltpu.VMEM((edev, 8 * cap, f), BF),
            pltpu.VMEM((edev, 8 * cap, kc), BF),
            pltpu.VMEM((4, edev * 2 * cap, 2 * b), BF),
            pltpu.VMEM((4, 6 * b, edev * 2 * cap), BF),
            pltpu.VMEM((NA, kc, 2 * f), BF),
            pltpu.VMEM((NB, f, NC), BF),
            pltpu.VMEM((4, edev * 2 * cap, NC), BF),
            pltpu.VMEM((b, 2 * f), F32),
            pltpu.VMEM((b, f), BF),
            pltpu.VMEM((nn, b, NC), F32),
            pltpu.VMEM((b, d), BF),
            pltpu.VMEM((nn, b, 4 * NC), F32),
            pltpu.VMEM((nn, b, NC), F32),
            pltpu.VMEM((nn, b, NC), F32),
            pltpu.VMEM((nn, b, NC), F32),
            pltpu.VMEM((8 * edev, b), F32),
            pltpu.VMEM((8 * edev, b), F32),
            dma((3,)), dma((NA, 2)), dma((NB,)),
            dma((nk, 4)), dma((nk, 4)), dma((nk, 3)), dma((nk, 3)), dma((7,)), dma((7,)),
            dma((nn,)), dma((nn,)), dma((nn,)), dma((nn,)), dma((nn,)), dma((nn,)), dma((nn,)), dma((nn,)),
        ],
        compiler_params=pltpu.CompilerParams(collective_id=0, has_side_effects=True, vmem_limit_bytes=67043328),
        name='moe',
    )(u, h, rt, ws1, ws3, ws2, w1, w3, w2)


def solution(mesh):
    ey, ex = mesh.shape['ey'], mesh.shape['ex']
    rows = P(('ey', 'ex'))
    rep = P()

    def local(x, kv_k, kv_v, lens, topk_idx, gates, ln1, ln2, wq, wo, ws1, ws3, ws2, w1, w3, w2):
        h, u, rt = _attn(x, kv_k, kv_v, lens, ln1, ln2, topk_idx, gates, wq, wo)
        return _moe(u, h, rt, ws1, ws3, ws2, w1, w3, w2, ey, ex)

    return jax.shard_map(
        local, mesh=mesh,
        in_specs=(rows, rows, rows, rows, rows, rows, rep, rep, rep, rep, rep, rep, rep, rows, rows, rows),
        out_specs=rows, check_vma=False)
```
